1024 devices in a mesh: gx: 16 (over z_lo, x), gy: 64 (over z_hi, y, core).
Axes of the slice: x: 4, y: 8, z: 16 (z_hi: 4, z_lo: 4; z = z_hi * 4 + z_lo), core: 2. Of those that a mesh axis runs over, the one named last changes fastest.
Arguments:
- velocity: float32 [3, 512, 512, 128], P(None, 'gx', 'gy'), may hold values from -6 to 6
- stress: float32 [6, 512, 512, 128], P(None, 'gx', 'gy'), may hold values from -6 to 6
- lame_first: float32 [512, 512, 128], P('gx', 'gy'), may hold values from 0.5 to 2
- modulus: float32 [512, 512, 128], P('gx', 'gy'), may hold values from 0.5 to 2
- buoyancy: float32 [512, 512, 128], P('gx', 'gy'), may hold values from 0.5 to 2
- zone: int32 [512, 512, 128], P('gx', 'gy'), may hold values from 0 to 7
- eligible: int32 [512, 512, 128], P('gx', 'gy'), may hold values 0 or 1
- cohesion: float32 [8], replicated, may hold values from 0.2 to 2
- friction: float32 [8], replicated, may hold values from 0.1 to 0.6
- source_cell: int32 [16], replicated, may hold values from 0 to 33554431
- source_moment: float32 [6, 16], replicated, may hold values from -15 to 15
Outputs:
- velocity_out: float32 [3, 512, 512, 128], P(None, 'gx', 'gy')
- stress_out: float32 [6, 512, 512, 128], P(None, 'gx', 'gy')
The draws below stay inside these ranges and needn't reach their ends.
All inputs are finite; a program needn't handle non-finite values. No bound on the sum of `eligible` on one device may be relied on, other than what follows from the above.
Results may differ from the reference program's by a relative error of at most 0.00011.
Values sent between devices are 32-bit elements; how exact they have to be, the bound alone decides.
A program may use at most 32 MiB of HBM per device.

```python
import math
import jax
import jax.numpy as jnp
from jax import lax

NZ = 128
STEPS = 2
NZONES = 8
NSRC = 16
NX = 512
NY = 512


def with_ends(values, stream_key, low, largest):
    longest = values.shape.index(max(values.shape))
    spots = []
    for shift in (0, 1):
        where = [jax.random.randint(jax.random.fold_in(stream_key, axis), (), 0, length) for axis, length in enumerate(values.shape)]
        where[longest] = (where[longest] + shift) % values.shape[longest]
        spots.append(tuple(where))
    return values.at[spots[0]].set(low).at[spots[1]].set(largest)


def levels(stream_key, shape, cuts, smallest, high):
    def one(position, parts):
        steps = jax.random.uniform(jax.random.fold_in(jax.random.fold_in(stream_key, 6), position), (parts,), jnp.float32, smallest / len(cuts), high / len(cuts))
        return jnp.repeat(jnp.exp(steps), shape[position] // parts).reshape((-1,) + (1,) * (len(shape) - position - 1))

    level = one(*cuts[0])
    for cut in cuts[1:]:
        level = level * one(*cut)
    return level


def centred(key, extent, deviation, most, pieces=(), dtype=jnp.bfloat16):
    array = jax.random.normal(key, extent, jnp.float32) * deviation
    if len(pieces) > 0:
        array = levels(key, extent, pieces, -0.22, 0.18) * array
    return jnp.clip(array, min=-most, max=most).astype(dtype)


def setup_inputs(seed: int = 0) -> dict:
    seeds = jax.random.split(jax.random.key(seed), 12)
    return {
        "velocity": centred(seeds[0], (3, NX, NY, NZ), 1.0, 6.0, ((1, 16), (2, 64)), jnp.float32),
        "stress": centred(seeds[1], (6, NX, NY, NZ), 1.0, 6.0, ((1, 16), (2, 64)), jnp.float32),
        "lame_first": jnp.clip(jnp.exp(math.log(2.0) - 1.3862944 * jax.random.uniform(seeds[2], (NX, NY, NZ), jnp.float32) ** levels(seeds[2], (NX, NY, NZ), ((0, 16), (1, 64)), -0.2, 0.2)), 0.5, 2.0),
        "modulus": jnp.clip(jnp.exp(math.log(2.0) - 1.3862944 * jax.random.uniform(seeds[3], (NX, NY, NZ), jnp.float32) ** levels(seeds[3], (NX, NY, NZ), ((0, 16), (1, 64)), -0.2, 0.2)), 0.5, 2.0),
        "buoyancy": jnp.clip(jnp.exp(math.log(2.0) - 1.3862944 * jax.random.uniform(seeds[4], (NX, NY, NZ), jnp.float32) ** levels(seeds[4], (NX, NY, NZ), ((0, 16), (1, 64)), -0.2, 0.2)), 0.5, 2.0),
        "zone": with_ends(jax.random.randint(seeds[5], (NX, NY, NZ), 0, NZONES), jax.random.fold_in(seeds[5], 1), 0, NZONES - 1).astype(jnp.int32),
        "eligible": with_ends((jax.random.randint(seeds[6], (NX, NY, NZ), 0, 2) < 1).astype(jnp.int32), jax.random.fold_in(seeds[6], 1), 0, 1),
        "cohesion": jnp.clip(jnp.exp(jax.random.uniform(seeds[7], (NZONES,), jnp.float32, math.log(0.2), math.log(2.0))), 0.2, 2.0),
        "friction": jnp.clip(jax.random.uniform(seeds[8], (NZONES,), jnp.float32, 0.1, 0.6), 0.1, 0.6),
        "source_cell": with_ends(jax.random.randint(seeds[9], (NSRC,), 0, NX * NY * NZ), jax.random.fold_in(seeds[9], 1), 0, (NX * NY * NZ) - 1).astype(jnp.int32),
        "source_moment": centred(seeds[10], (6, NSRC), 3.0, 15.0, (), jnp.float32),
    }


time_step = 0.1
near_weight = 9.0 / 8.0
far_weight = 1.0 / 24.0
shear_floor = 0.25

def crop(padded, axis, offset):
    result = padded
    for dim in range(3):
        begin = offset if dim == axis else 2
        length = padded.shape[dim] - 4
        result = lax.slice_in_dim(result, begin, begin + length, axis=dim)
    return result

def derivative(padded, axis, forward):
    if forward:
        return near_weight * (crop(padded, axis, 3) - crop(padded, axis, 2)) - far_weight * (crop(padded, axis, 4) - crop(padded, axis, 1))
    return near_weight * (crop(padded, axis, 2) - crop(padded, axis, 1)) - far_weight * (crop(padded, axis, 3) - crop(padded, axis, 0))

def velocity_update(stress_pad, velocity, buoyancy):
    force_x = derivative(stress_pad[0], 0, True) + derivative(stress_pad[3], 1, False) + derivative(stress_pad[4], 2, False)
    force_y = derivative(stress_pad[3], 0, False) + derivative(stress_pad[1], 1, True) + derivative(stress_pad[5], 2, False)
    force_z = derivative(stress_pad[4], 0, False) + derivative(stress_pad[5], 1, False) + derivative(stress_pad[2], 2, True)
    forces = jnp.stack([force_x, force_y, force_z])
    return velocity + time_step * buoyancy[None] * forces

def stress_update(flow_pad, stress, lame_first, modulus):
    strain_x = derivative(flow_pad[0], 0, False)
    strain_y = derivative(flow_pad[1], 1, False)
    strain_z = derivative(flow_pad[2], 2, False)
    dilation = strain_x + strain_y + strain_z
    shear_xy = derivative(flow_pad[0], 1, True) + derivative(flow_pad[1], 0, True)
    shear_xz = derivative(flow_pad[0], 2, True) + derivative(flow_pad[2], 0, True)
    shear_yz = derivative(flow_pad[1], 2, True) + derivative(flow_pad[2], 1, True)
    rates = jnp.stack([lame_first * dilation + 2.0 * modulus * strain_x, lame_first * dilation + 2.0 * modulus * strain_y, lame_first * dilation + 2.0 * modulus * strain_z, modulus * shear_xy, modulus * shear_xz, modulus * shear_yz])
    return stress + time_step * rates

def plastic(stress, cell_cohesion, cell_friction, eligible):
    pressure = (stress[0] + stress[1] + stress[2]) / 3.0
    dev_x = stress[0] - pressure
    dev_y = stress[1] - pressure
    dev_z = stress[2] - pressure
    second = 0.5 * (dev_x * dev_x + dev_y * dev_y + dev_z * dev_z) + stress[3] * stress[3] + stress[4] * stress[4] + stress[5] * stress[5]
    strength = jnp.maximum(cell_cohesion * jnp.sqrt(1.0 - cell_friction * cell_friction) - pressure * cell_friction, 0.0)
    ratio = jnp.minimum(1.0, strength / jnp.maximum(jnp.sqrt(second), shear_floor))
    factor = jnp.where(eligible == 1, ratio, 1.0)
    return jnp.stack([pressure + factor * dev_x, pressure + factor * dev_y, pressure + factor * dev_z, factor * stress[3], factor * stress[4], factor * stress[5]])

def pad_space(field, width):
    return jnp.pad(field, ((0, 0), (width, width), (width, width), (width, width)))

def reference(velocity, stress, lame_first, modulus, buoyancy, zone, eligible, cohesion, friction, source_cell, source_moment):
    cell_cohesion = cohesion[zone]
    cell_friction = friction[zone]
    plane = NY * NZ
    src_x = (source_cell // plane).astype(jnp.int32)
    src_y = (source_cell // NZ % NY).astype(jnp.int32)
    src_z = (source_cell % NZ).astype(jnp.int32)
    injection = jnp.zeros_like(stress).at[:, src_x, src_y, src_z].add(time_step * source_moment)
    for step in range(STEPS):
        velocity = velocity_update(pad_space(stress, 2), velocity, buoyancy)
        stress = stress_update(pad_space(velocity, 2), stress, lame_first, modulus)
        stress = stress + injection
        stress = plastic(stress, cell_cohesion, cell_friction, eligible)
    return (velocity, stress)
```

```python
import functools

import jax
import jax.numpy as jnp
from jax import lax
from jax.experimental import pallas as pl
from jax.experimental.pallas import tpu as pltpu
from jax.sharding import PartitionSpec as P

STEPS = 2
TIME_STEP = 0.1
MESH = pl.DeviceIdType.MESH
NX, NY, NZ = 32, 8, 128
PITCH = 24
EXT = (NX + 4) * PITCH
TILES = 4

WEIGHT = {"F": {1: 27.0, 0: -27.0, 2: -1.0, -1: 1.0}, "B": {0: 27.0, -1: -27.0, 1: -1.0, -2: 1.0}}
LOW = {"F": (-1,), "B": (-2, -1)}
HIGH = {"F": (0, 1), "B": (0,)}
FORCE_X = ((0, "F"), (3, "B"), (4, "B"))
FORCE_Y = ((3, "B"), (1, "F"), (5, "B"))
FORCE_Z = ((4, "B"), (5, "B"), (2, "F"))
FLOW_X = ((0, "B"), (1, "F"), (2, "F"))
FLOW_Y = ((0, "F"), (1, "B"), (2, "F"))
FLOW_Z = ((0, "F"), (1, "F"), (2, "B"))


def layers(table, side):
    return [(field, layer) for field, kind in table for layer in side[kind]]


STRESS_Y = (layers(FORCE_Y, HIGH), layers(FORCE_Y, LOW))
STRESS_X = (layers(FORCE_X, HIGH), layers(FORCE_X, LOW))
FLOW_SENT_Y = (layers(FLOW_Y, HIGH), layers(FLOW_Y, LOW))
FLOW_SENT_X = (layers(FLOW_X, HIGH), layers(FLOW_X, LOW))
LIGHT = ((0, 1), (-2, -1))

YS, YP, XS, XV = range(4)
COUNTS = {
    YS: tuple(len(STRESS_Y[d]) for d in (0, 1)),
    YP: tuple(len(FLOW_SENT_Y[d]) for d in (0, 1)),
    XS: tuple(len(STRESS_X[d]) for d in (0, 1)),
    XV: tuple(len(FLOW_SENT_X[d]) for d in (0, 1)),
}


def message_rows(step, kind, direction):
    count = COUNTS[kind][direction]
    if kind == YS and step == 0:
        count += 2
    return count * (NX if kind in (YS, YP) else NY)


MESSAGES = [(s, k, d) for s in range(STEPS) for k in range(4) for d in (0, 1)]


def kernel(
    velocity,
    stress,
    lame_hbm,
    modulus_hbm,
    buoyancy_hbm,
    zone_hbm,
    eligible_hbm,
    cohesion_hbm,
    friction_hbm,
    cell_hbm,
    moment_hbm,
    velocity_out,
    stress_out,
    s_in,
    v_in,
    lame,
    modulus,
    buoyancy,
    zone,
    eligible,
    cohesion,
    friction,
    cell,
    moment,
    s_ext,
    v_ext,
    strength,
    slope,
    inject,
    v_res,
    s_res,
    *rest,
):
    sent = dict(zip(MESSAGES, rest[: len(MESSAGES)]))
    got = dict(zip(MESSAGES, rest[len(MESSAGES) : 2 * len(MESSAGES)]))
    load_sem, store_sem, send_sem, recv_sem = rest[2 * len(MESSAGES) :]
    gx, gy = lax.axis_index("gx"), lax.axis_index("gy")
    size_x, size_y = lax.axis_size("gx"), lax.axis_size("gy")

    there = {"x": (gx > 0, gx < size_x - 1), "y": (gy > 0, gy < size_y - 1)}
    target = {
        "x": ({"gx": gx - 1}, {"gx": gx + 1}),
        "y": ({"gy": gy - 1}, {"gy": gy + 1}),
    }

    barrier = pltpu.get_barrier_semaphore()
    for axis in "yx":
        for d in (0, 1):

            @pl.when(there[axis][d])
            def _():
                pl.semaphore_signal(
                    barrier, inc=1, device_id=target[axis][d], device_id_type=MESH
                )

    loads = [
        pltpu.make_async_copy(a, b, load_sem.at[i])
        for i, (a, b) in enumerate(
            (
                (stress, s_in),
                (buoyancy_hbm, buoyancy),
                (velocity, v_in),
                (zone_hbm, zone),
                (eligible_hbm, eligible),
                (lame_hbm, lame),
                (modulus_hbm, modulus),
                (cohesion_hbm, cohesion),
                (friction_hbm, friction),
                (cell_hbm, cell),
                (moment_hbm, moment),
            )
        )
    ]
    for load in loads:
        load.start()

    def axis_of(kind):
        return "y" if kind in (YS, YP) else "x"

    def remote(step, kind, d):
        at = MESSAGES.index((step, kind, d))
        return pltpu.make_async_remote_copy(
            src_ref=sent[step, kind, d],
            dst_ref=got[step, kind, d],
            send_sem=send_sem.at[at],
            recv_sem=recv_sem.at[at],
            device_id=target[axis_of(kind)][d],
            device_id_type=MESH,
        )

    def send(step, kind):
        for d in (0, 1):

            @pl.when(there[axis_of(kind)][d])
            def _():
                remote(step, kind, d).start()

    def receive(step, kind):
        for d in (0, 1):

            @pl.when(there[axis_of(kind)][1 - d])
            def _():
                remote(step, kind, d).wait_recv()

    for axis in "xy":
        for d in (0, 1):

            @pl.when(jnp.logical_not(there[axis][1 - d]))
            def _():
                for step, kind, way in MESSAGES:
                    if way == d and axis_of(kind) == axis:
                        ref = got[step, kind, way]
                        ref[...] = jnp.zeros(ref.shape, jnp.float32)

    zero = jnp.zeros((NY, NZ), jnp.float32)
    for field in (0, 3, 4):
        for x in (-2, -1, NX, NX + 1):
            s_ext[field, pl.ds((x + 2) * PITCH + NY, NY), :] = zero

    def clear(x, _):
        for field in (1, 3, 5):
            for offset in (0, 2 * NY):
                start = pl.multiple_of((x + 2) * PITCH + offset, NY)
                s_ext[field, pl.ds(start, NY), :] = zero
        return _

    lax.fori_loop(0, NX, clear, 0)

    lane = lax.broadcasted_iota(jnp.int32, (NY, NZ), 1)
    keep = {1: lane < NZ - 1, 2: lane < NZ - 2, -1: lane >= 1, -2: lane >= 2}

    def weighted(terms):
        total = None
        for weight, value in terms:
            if weight < 0 and total is not None:
                total = total - (value if weight == -1.0 else -weight * value)
            else:
                value = value if weight == 1.0 else weight * value
                total = value if total is None else total + value
        return total

    def spread(kind, at):
        if kind == "F":
            return 27.0 * (at(1) - at(0)) - (at(2) - at(-1))
        return 27.0 * (at(0) - at(-1)) - (at(1) - at(-2))

    def along_x(ref, field, kind, base):
        return spread(
            kind,
            lambda o: ref[field, pl.ds(pl.multiple_of(base + o * PITCH, NY), NY), :],
        )

    def along_y(ref, field, kind, base):
        return spread(
            kind,
            lambda o: ref[
                field, pl.ds(pl.multiple_of(base, NY) if o == 0 else base + o, NY), :
            ],
        )

    def along_z(ref, field, kind, base):
        value = ref[field, pl.ds(pl.multiple_of(base, NY), NY), :]

        def at(o):
            if o == 0:
                return value
            return jnp.where(keep[o], pltpu.roll(value, (-o) % NZ, 1), 0.0)

        return spread(kind, at)

    def place(x):
        return pl.multiple_of(x * NY, NY), (x + 2) * PITCH + NY

    def columns(row):
        return pl.ds(2 * PITCH + NY + row, NX, stride=PITCH)

    def part(ref, at, rows):
        return ref[pl.ds(at * rows, rows), :]


    def pack_stress(step):
        for d in (0, 1):
            base = NY if d else 0
            out = sent[step, YS, d]
            for at, (field, layer) in enumerate(STRESS_Y[d]):
                if step == 0:
                    value = s_in[field, pl.ds(base + layer, NX, stride=NY), :]
                else:
                    value = s_ext[field, columns(base + layer), :]
                out[pl.ds(at * NX, NX), :] = value
            if step == 0:
                for at, layer in enumerate(LIGHT[d]):
                    out[pl.ds((len(STRESS_Y[d]) + at) * NX, NX), :] = buoyancy[
                        pl.ds(base + layer, NX, stride=NY), :
                    ]
            base = NX if d else 0
            out = sent[step, XS, d]
            for at, (field, layer) in enumerate(STRESS_X[d]):
                x = base + layer
                if step == 0:
                    value = s_in[field, pl.ds(x * NY, NY), :]
                else:
                    value = s_ext[field, pl.ds((x + 2) * PITCH + NY, NY), :]
                out[pl.ds(at * NY, NY), :] = value

    def extend(k, _):
        for j in range(TILES):
            row, base = place(k * TILES + j)
            for field in range(6):
                s_ext[field, pl.ds(pl.multiple_of(base, NY), NY), :] = s_in[
                    field, pl.ds(row, NY), :
                ]
        return _

    def move(step):
        def body(k, _):
            for j in range(TILES):
                row, base = place(k * TILES + j)
                light = (TIME_STEP / 24.0) * buoyancy[pl.ds(row, NY), :]
                main = pl.ds(pl.multiple_of(base, NY), NY)
                for c in range(3):
                    force = along_x(s_ext, *FORCE_X[c], base)
                    force += along_y(s_ext, *FORCE_Y[c], base)
                    force += along_z(s_ext, *FORCE_Z[c], base)
                    old = v_in[c, pl.ds(row, NY), :] if step == 0 else v_ext[c, main, :]
                    v_ext[c, main, :] = old + light * force
            return _

        lax.fori_loop(0, NX // TILES, body, 0)

    def beyond(kind, low, i, count):
        if low:
            return [(WEIGHT[kind][r - i], r) for r in LOW[kind] if r - i in WEIGHT[kind]]
        return [
            (WEIGHT[kind][count + r - i], r) for r in HIGH[kind] if count + r - i in WEIGHT[kind]
        ]

    def mend_x(step):
        for low in (True, False):
            d = 1 if low else 0
            halo = got[step, XS, d]
            for i in (0, 1) if low else (NX - 2, NX - 1):
                light = (TIME_STEP / 24.0) * buoyancy[pl.ds(i * NY, NY), :]
                for c, (field, kind) in enumerate(FORCE_X):
                    terms = beyond(kind, low, i, NX)
                    if terms:
                        main = pl.ds((i + 2) * PITCH + NY, NY)
                        v_ext[c, main, :] += light * weighted(
                            [
                                (w, part(halo, STRESS_X[d].index((field, r)), NY))
                                for w, r in terms
                            ]
                        )

    def pack_flow_y(step):
        for d in (0, 1):
            base = NY if d else 0
            for at, (c, layer) in enumerate(FLOW_SENT_Y[d]):
                sent[step, YP, d][pl.ds(at * NX, NX), :] = v_ext[c, columns(base + layer), :]

    def mend_y(step):
        for low in (True, False):
            d = 1 if low else 0
            halo = got[step, YS, d]
            mine = sent[0, YS, 1 - d]
            for at, layer in enumerate(LIGHT[1 - d]):
                i = layer if low else NY + layer
                light = (TIME_STEP / 24.0) * part(mine, len(STRESS_Y[1 - d]) + at, NX)
                for c, (field, kind) in enumerate(FORCE_Y):
                    terms = beyond(kind, low, i, NY)
                    if terms:
                        v_ext[c, columns(i), :] += light * weighted(
                            [
                                (w, part(halo, STRESS_Y[d].index((field, r)), NX))
                                for w, r in terms
                            ]
                        )

    def pack_flow_x(step):
        for d in (0, 1):
            base = NX if d else 0
            for at, (c, layer) in enumerate(FLOW_SENT_X[d]):
                sent[step, XV, d][pl.ds(at * NY, NY), :] = v_ext[
                    c, pl.ds((base + layer + 2) * PITCH + NY, NY), :
                ]

    def finish_y(step):
        for low in (True, False):
            d = 1 if low else 0
            flow = got[step, YP, d]
            first = got[0, YS, d]
            own = sent[step, YS, 1 - d]
            for at, (c, layer) in enumerate(FLOW_SENT_Y[d]):
                light = (TIME_STEP / 24.0) * part(
                    first, len(STRESS_Y[d]) + LIGHT[d].index(layer), NX
                )
                field, kind = FORCE_Y[c]
                side = HIGH[kind] if low else LOW[kind]
                terms = [
                    (WEIGHT[kind][j - layer], part(own, STRESS_Y[1 - d].index((field, j)), NX))
                    for j in side
                    if j - layer in WEIGHT[kind]
                ]
                value = part(flow, at, NX)
                if terms:
                    value = value + light * weighted(terms)
                v_ext[c, columns(layer if low else NY + layer), :] = value

    def finish_x(step):
        for low in (True, False):
            d = 1 if low else 0
            for at, (c, layer) in enumerate(FLOW_SENT_X[d]):
                x = layer if low else NX + layer
                v_ext[c, pl.ds((x + 2) * PITCH + NY, NY), :] = part(got[step, XV, d], at, NY)

    def stress_layer(step, x):
        row, base = place(x)
        main = pl.ds(pl.multiple_of(base, NY), NY)
        here = pl.ds(row, NY)
        mu = (TIME_STEP / 24.0) * modulus[here, :]
        lam = (TIME_STEP / 24.0) * lame[here, :]
        e_x = along_x(v_ext, 0, "B", base)
        e_y = along_y(v_ext, 1, "B", base)
        e_z = along_z(v_ext, 2, "B", base)
        dilation = lam * (e_x + e_y + e_z)
        twice = mu + mu
        rates = (
            dilation + twice * e_x,
            dilation + twice * e_y,
            dilation + twice * e_z,
            mu * (along_y(v_ext, 0, "F", base) + along_x(v_ext, 1, "F", base)),
            mu * (along_z(v_ext, 0, "F", base) + along_x(v_ext, 2, "F", base)),
            mu * (along_z(v_ext, 1, "F", base) + along_y(v_ext, 2, "F", base)),
        )
        s = [s_ext[f, main, :] + (rates[f] + inject[f, here, :]) for f in range(6)]
        pressure = (s[0] + s[1] + s[2]) * (1.0 / 3.0)
        d = [s[f] - pressure for f in range(3)]
        second = 0.5 * (d[0] * d[0] + d[1] * d[1] + d[2] * d[2])
        second = second + s[3] * s[3] + s[4] * s[4] + s[5] * s[5]
        limit = jnp.maximum(strength[here, :] - pressure * slope[here, :], 0.0)
        ratio = limit * lax.rsqrt(jnp.maximum(second, 0.0625))
        factor = jnp.where(eligible[here, :] == 1, jnp.minimum(ratio, 1.0), 1.0)
        new = [pressure + factor * d[f] for f in range(3)] + [factor * s[f] for f in (3, 4, 5)]
        for f in range(6):
            if step == STEPS - 1:
                s_res[f, here, :] = new[f]
            else:
                s_ext[f, main, :] = new[f]

    def deform(step, start, stride, steps):
        def body(k, _):
            for j in range(2):
                stress_layer(step, start + k * stride + j)
            return _

        lax.fori_loop(0, steps, body, 0)

    def prepare():
        row = lax.broadcasted_iota(jnp.int32, (NY, NZ), 0)
        total_y = size_y * NY
        corner = ((gx * NX) * total_y + gy * NY) * NZ
        within = row * NZ + lane

        def body(x, _):
            here = pl.ds(pl.multiple_of(x * NY, NY), NY)
            which = zone[here, :]
            coh = jnp.full((NY, NZ), cohesion[0], jnp.float32)
            fri = jnp.full((NY, NZ), friction[0], jnp.float32)
            for z in range(1, 8):
                hit = which == z
                coh = jnp.where(hit, cohesion[z], coh)
                fri = jnp.where(hit, friction[z], fri)
            strength[here, :] = coh * jnp.sqrt(1.0 - fri * fri)
            slope[here, :] = fri
            index = within + (corner + x * (total_y * NZ))
            sums = [zero] * 6
            for source in range(16):
                hit = index == cell[source]
                for f in range(6):
                    sums[f] = sums[f] + jnp.where(hit, TIME_STEP * moment[f, source], 0.0)
            for f in range(6):
                inject[f, here, :] = sums[f]
            return _

        lax.fori_loop(0, NX, body, 0)


    for load in loads[:2]:
        load.wait()
    pack_stress(0)
    expected = sum(t.astype(jnp.int32) for axis in "xy" for t in there[axis])
    pl.semaphore_wait(barrier, expected)
    stores = []
    for step in range(STEPS):
        if step:
            pack_stress(step)
        send(step, YS)
        send(step, XS)
        if step == 0:
            lax.fori_loop(0, NX // TILES, extend, 0)
            loads[2].wait()
        move(step)
        receive(step, XS)
        mend_x(step)
        pack_flow_y(step)
        send(step, YP)
        if step == 0:
            for load in loads[3:]:
                load.wait()
            prepare()
        receive(step, YS)
        mend_y(step)
        pack_flow_x(step)
        send(step, XV)
        if step == STEPS - 1:

            def keep_flow(k, _):
                for j in range(TILES):
                    row, base = place(k * TILES + j)
                    for c in range(3):
                        v_res[c, pl.ds(row, NY), :] = v_ext[
                            c, pl.ds(pl.multiple_of(base, NY), NY), :
                        ]
                return _

            lax.fori_loop(0, NX // TILES, keep_flow, 0)
            store = pltpu.make_async_copy(v_res, velocity_out, store_sem.at[0])
            store.start()
            stores.append(store)
        receive(step, YP)
        finish_y(step)
        deform(step, 2, 2, (NX - 4) // 2)
        if step == STEPS - 1:
            inner = pl.ds(2 * NY, (NX - 4) * NY)
            store = pltpu.make_async_copy(
                s_res.at[:, inner], stress_out.at[:, inner], store_sem.at[1]
            )
            store.start()
            stores.append(store)
        receive(step, XV)
        finish_x(step)
        deform(step, 0, NX - 2, 2)
    for at, start in ((2, 0), (3, (NX - 2) * NY)):
        edge = pl.ds(start, 2 * NY)
        store = pltpu.make_async_copy(s_res.at[:, edge], stress_out.at[:, edge], store_sem.at[at])
        store.start()
        stores.append(store)
    for store in stores:
        store.wait()
    for step, kind, d in MESSAGES:

        @pl.when(there[axis_of(kind)][d])
        def _():
            remote(step, kind, d).wait_send()


def on_device(velocity, stress, lame, modulus, buoyancy, zone, eligible, *tables):
    rows = NX * NY
    flat = [a.reshape(a.shape[:-3] + (rows, NZ)) for a in (velocity, stress, lame, modulus, buoyancy, zone, eligible)]
    f32 = jnp.float32
    hbm = pl.BlockSpec(memory_space=pl.ANY)
    buffers = [
        pltpu.VMEM((message_rows(*m), NZ), f32) for m in MESSAGES
    ]
    block = pltpu.VMEM((rows, NZ), f32)
    whole = pltpu.VMEM((rows, NZ), jnp.int32)
    v, s = pl.pallas_call(
        kernel,
        out_shape=(
            jax.ShapeDtypeStruct((3, rows, NZ), f32),
            jax.ShapeDtypeStruct((6, rows, NZ), f32),
        ),
        in_specs=[hbm] * 11,
        out_specs=(hbm, hbm),
        scratch_shapes=[
            pltpu.VMEM((6, rows, NZ), f32),
            pltpu.VMEM((3, rows, NZ), f32),
            block,
            block,
            block,
            whole,
            whole,
            pltpu.SMEM((8,), f32),
            pltpu.SMEM((8,), f32),
            pltpu.SMEM((16,), jnp.int32),
            pltpu.SMEM((6, 16), f32),
            pltpu.VMEM((6, EXT, NZ), f32),
            pltpu.VMEM((3, EXT, NZ), f32),
            block,
            block,
            pltpu.VMEM((6, rows, NZ), f32),
            pltpu.VMEM((3, rows, NZ), f32),
            pltpu.VMEM((6, rows, NZ), f32),
            *buffers,
            *buffers,
            pltpu.SemaphoreType.DMA((11,)),
            pltpu.SemaphoreType.DMA((4,)),
            pltpu.SemaphoreType.DMA((len(MESSAGES),)),
            pltpu.SemaphoreType.DMA((len(MESSAGES),)),
        ],
        compiler_params=pltpu.CompilerParams(collective_id=0, has_side_effects=True),
    )(*flat, *tables)
    return v.reshape(velocity.shape), s.reshape(stress.shape)


def solution(mesh):
    wide, field, table = P(None, "gx", "gy", None), P("gx", "gy", None), P()
    return jax.shard_map(
        on_device,
        mesh=mesh,
        in_specs=(wide, wide) + (field,) * 5 + (table,) * 4,
        out_specs=(wide, wide),
        check_vma=False,
    )
```

```python
import functools

import jax
import jax.numpy as jnp
from jax import lax
from jax.experimental import pallas as pl
from jax.experimental.pallas import tpu as pltpu
from jax.sharding import PartitionSpec as P

STEPS = 2
TIME_STEP = 0.1
MESH = pl.DeviceIdType.MESH
NX, NY, NZ = 32, 8, 128
PITCH = 24
EXT = (NX + 4) * PITCH
TILES = 4

WEIGHT = {"F": {1: 27.0, 0: -27.0, 2: -1.0, -1: 1.0}, "B": {0: 27.0, -1: -27.0, 1: -1.0, -2: 1.0}}
LOW = {"F": (-1,), "B": (-2, -1)}
HIGH = {"F": (0, 1), "B": (0,)}
FORCE_X = ((0, "F"), (3, "B"), (4, "B"))
FORCE_Y = ((3, "B"), (1, "F"), (5, "B"))
FORCE_Z = ((4, "B"), (5, "B"), (2, "F"))
FLOW_X = ((0, "B"), (1, "F"), (2, "F"))
FLOW_Y = ((0, "F"), (1, "B"), (2, "F"))
FLOW_Z = ((0, "F"), (1, "F"), (2, "B"))


def layers(table, side):
    return [(field, layer) for field, kind in table for layer in side[kind]]


STRESS_Y = (layers(FORCE_Y, HIGH), layers(FORCE_Y, LOW))
STRESS_X = (layers(FORCE_X, HIGH), layers(FORCE_X, LOW))
FLOW_SENT_Y = (layers(FLOW_Y, HIGH), layers(FLOW_Y, LOW))
FLOW_SENT_X = (layers(FLOW_X, HIGH), layers(FLOW_X, LOW))
LIGHT = ((0, 1), (-2, -1))

YS, YP, XS, XP, CORNER = range(5)
COUNTS = {
    YS: tuple(len(STRESS_Y[d]) for d in (0, 1)),
    YP: tuple(len(FLOW_SENT_Y[d]) for d in (0, 1)),
    XS: tuple(len(STRESS_X[d]) for d in (0, 1)),
    XP: tuple(len(FLOW_SENT_X[d]) for d in (0, 1)),
}


def beyond(kind, low, i, count):
    if low:
        return [(WEIGHT[kind][r - i], r) for r in LOW[kind] if r - i in WEIGHT[kind]]
    return [(WEIGHT[kind][count + r - i], r) for r in HIGH[kind] if count + r - i in WEIGHT[kind]]


def corner(direction):
    up_x, up_y = divmod(direction, 2)
    base_x, base_y = NX * up_x, NY * up_y
    along_y, along_x = [], []
    for c, layer in FLOW_SENT_Y[up_y]:
        field, kind = FORCE_X[c]
        for i in (0, 1) if up_x else (NX - 2, NX - 1):
            terms = beyond(kind, up_x, i, NX)
            if terms:
                along_y.append((c, layer, i, [(w, field, base_x + r, base_y + layer) for w, r in terms]))
    for c, layer in FLOW_SENT_X[up_x]:
        field, kind = FORCE_Y[c]
        for i in (0, 1) if up_y else (NY - 2, NY - 1):
            terms = beyond(kind, up_y, i, NY)
            if terms:
                along_x.append((c, layer, i, [(w, field, base_x + layer, base_y + r) for w, r in terms]))
    return along_y, along_x


def message_rows(step, kind, direction):
    if kind == CORNER:
        return 2 * NY
    count = COUNTS[kind][direction]
    if kind in (YS, XS) and step == 0:
        count += 2
    return count * (NX if kind in (YS, YP) else NY)


RUN = 16
SENDER = (0, RUN - 1)
RELAY = ((RUN - 1, 3), (1, RUN - 3))
PARTS = 1 + len(RELAY[0])


def part_rows(step, kind, direction):
    rows = message_rows(step, kind, direction)
    each = rows // PARTS // NY * NY
    cuts = [0] + [rows - each * (PARTS - 1 - p) for p in range(PARTS)]
    return [pl.ds(a, b - a) for a, b in zip(cuts, cuts[1:])]


MESSAGES = [
    (s, k, d) for s in range(STEPS) for k in range(5) for d in range(4 if k == CORNER else 2)
]
PASSING = [(s, k) for s in range(STEPS) for k in (YS, YP)] if PARTS > 1 else []


def passing_rows(step, kind):
    return max(r.size for d in (0, 1) for r in part_rows(step, kind, d)[1:])


def kernel(
    velocity,
    stress,
    lame_hbm,
    modulus_hbm,
    buoyancy_hbm,
    zone_hbm,
    eligible_hbm,
    cohesion_hbm,
    friction_hbm,
    cell_hbm,
    moment_hbm,
    velocity_out,
    stress_out,
    s_in,
    v_in,
    lame,
    modulus,
    buoyancy,
    zone,
    eligible,
    cohesion,
    friction,
    cell,
    moment,
    s_ext,
    v_ext,
    strength,
    slope,
    inject,
    *rest,
):
    sent = dict(zip(MESSAGES, rest[: len(MESSAGES)]))
    got = dict(zip(MESSAGES, rest[len(MESSAGES) : 2 * len(MESSAGES)]))
    rest = rest[2 * len(MESSAGES) :]
    passing = dict(zip(PASSING, rest[: len(PASSING)]))
    load_sem, send_sem, recv_sem, pass_sem, onward_sem = rest[len(PASSING) :]
    gx, gy = lax.axis_index("gx"), lax.axis_index("gy")
    size_x, size_y = lax.axis_size("gx"), lax.axis_size("gy")

    there = {"x": (gx > 0, gx < size_x - 1), "y": (gy > 0, gy < size_y - 1)}
    there["xy"] = [a & b for a in there["x"] for b in there["y"]]
    target = {
        "x": ({"gx": gx - 1}, {"gx": gx + 1}),
        "y": ({"gy": gy - 1}, {"gy": gy + 1}),
        "xy": [{"gx": gx + a, "gy": gy + b} for a in (-1, 1) for b in (-1, 1)],
    }
    ways = {"x": (0, 1), "y": (0, 1), "xy": range(4)}

    run, spot = gy // RUN, gy % RUN
    beyond_run = (run > 0, run < size_y // RUN - 1)
    crosses = [beyond_run[d] & (spot == SENDER[d]) for d in (0, 1)]
    relays = [
        (d, p, beyond_run[d] & (spot == RELAY[d][p - 1])) for d in (0, 1) for p in range(1, PARTS)
    ]

    barrier = pltpu.get_barrier_semaphore()
    for d, _, mine in relays:

        @pl.when(mine)
        def _():
            pl.semaphore_signal(
                barrier, inc=1, device_id={"gy": run * RUN + SENDER[d]}, device_id_type=MESH
            )
    for axis in ("y", "xy", "x"):
        for d in ways[axis]:

            @pl.when(there[axis][d])
            def _():
                pl.semaphore_signal(
                    barrier, inc=1, device_id=target[axis][d], device_id_type=MESH
                )

    loads = [
        pltpu.make_async_copy(a, b, load_sem.at[i])
        for i, (a, b) in enumerate(
            (
                (stress, s_in),
                (buoyancy_hbm, buoyancy),
                (velocity, v_in),
                (zone_hbm, zone),
                (eligible_hbm, eligible),
                (lame_hbm, lame),
                (modulus_hbm, modulus),
                (cohesion_hbm, cohesion),
                (friction_hbm, friction),
                (cell_hbm, cell),
                (moment_hbm, moment),
            )
        )
    ]
    for load in loads:
        load.start()

    def axis_of(kind):
        return {YS: "y", YP: "y", XS: "x", XP: "x", CORNER: "xy"}[kind]

    def remote(step, kind, d):
        at = MESSAGES.index((step, kind, d))
        return pltpu.make_async_remote_copy(
            src_ref=sent[step, kind, d],
            dst_ref=got[step, kind, d],
            send_sem=send_sem.at[at],
            recv_sem=recv_sem.at[at],
            device_id=target[axis_of(kind)][d],
            device_id_type=MESH,
        )

    def cut(step, kind, d, p):
        at = MESSAGES.index((step, kind, d))
        rows = part_rows(step, kind, d)[p]
        if p == 0:
            into, sem, where = got[step, kind, d].at[rows], recv_sem.at[at], target["y"][d]
        else:
            into = passing[step, kind].at[pl.ds(0, rows.size)]
            sem = pass_sem.at[PASSING.index((step, kind))]
            where = {"gy": run * RUN + RELAY[d][p - 1]}
        return pltpu.make_async_remote_copy(
            src_ref=sent[step, kind, d].at[rows],
            dst_ref=into,
            send_sem=send_sem.at[at],
            recv_sem=sem,
            device_id=where,
            device_id_type=MESH,
        )

    def onward(step, kind, d, p):
        rows = part_rows(step, kind, d)[p]
        return pltpu.make_async_remote_copy(
            src_ref=passing[step, kind].at[pl.ds(0, rows.size)],
            dst_ref=got[step, kind, d].at[rows],
            send_sem=onward_sem.at[PASSING.index((step, kind))],
            recv_sem=recv_sem.at[MESSAGES.index((step, kind, d))],
            device_id={"gy": (run + (1 if d else -1)) * RUN + SENDER[1 - d]},
            device_id_type=MESH,
        )

    def relay(step):
        for d, p, mine in relays:

            @pl.when(mine)
            def _():
                for kind in (YS, YP):
                    cut(step, kind, d, p).wait_recv()
                    onward(step, kind, d, p).start()

    def send(step, kind):
        axis = axis_of(kind)
        for d in ways[axis]:
            if axis != "y":

                @pl.when(there[axis][d])
                def _():
                    remote(step, kind, d).start()

            else:

                @pl.when(there["y"][d] & jnp.logical_not(crosses[d]))
                def _():
                    remote(step, kind, d).start()

                @pl.when(crosses[d])
                def _():
                    for p in reversed(range(PARTS)):
                        cut(step, kind, d, p).start()

    def receive(step, kind):
        axis = axis_of(kind)
        for d in ways[axis]:

            @pl.when(there[axis][ways[axis][-1] - d])
            def _():
                remote(step, kind, d).wait_recv()

    for axis in ways:
        for d in ways[axis]:

            @pl.when(jnp.logical_not(there[axis][ways[axis][-1] - d]))
            def _():
                for step, kind, way in MESSAGES:
                    if way == d and axis_of(kind) == axis:
                        ref = got[step, kind, way]
                        ref[...] = jnp.zeros(ref.shape, jnp.float32)

    zero = jnp.zeros((NY, NZ), jnp.float32)
    for field in (0, 3, 4):
        for x in (-2, -1, NX, NX + 1):
            s_ext[field, pl.ds((x + 2) * PITCH + NY, NY), :] = zero

    def clear(x, _):
        for field in (1, 3, 5):
            for offset in (0, 2 * NY):
                start = pl.multiple_of((x + 2) * PITCH + offset, NY)
                s_ext[field, pl.ds(start, NY), :] = zero
        return _

    lax.fori_loop(0, NX, clear, 0)

    lane = lax.broadcasted_iota(jnp.int32, (NY, NZ), 1)
    keep = {1: lane < NZ - 1, 2: lane < NZ - 2, -1: lane >= 1, -2: lane >= 2}

    def weighted(terms):
        total = None
        for weight, value in terms:
            if weight < 0 and total is not None:
                total = total - (value if weight == -1.0 else -weight * value)
            else:
                value = value if weight == 1.0 else weight * value
                total = value if total is None else total + value
        return total

    def spread(kind, at):
        if kind == "F":
            return 27.0 * (at(1) - at(0)) - (at(2) - at(-1))
        return 27.0 * (at(0) - at(-1)) - (at(1) - at(-2))

    def along_x(ref, field, kind, base):
        return spread(
            kind,
            lambda o: ref[field, pl.ds(pl.multiple_of(base + o * PITCH, NY), NY), :],
        )

    def along_y(ref, field, kind, base):
        return spread(
            kind,
            lambda o: ref[
                field, pl.ds(pl.multiple_of(base, NY) if o == 0 else base + o, NY), :
            ],
        )

    def along_z(ref, field, kind, base):
        value = ref[field, pl.ds(pl.multiple_of(base, NY), NY), :]

        def at(o):
            if o == 0:
                return value
            return jnp.where(keep[o], pltpu.roll(value, (-o) % NZ, 1), 0.0)

        return spread(kind, at)

    def place(x):
        return pl.multiple_of(x * NY, NY), (x + 2) * PITCH + NY

    def columns(row):
        return pl.ds(2 * PITCH + NY + row, NX, stride=PITCH)

    def part(ref, at, rows):
        return ref[pl.ds(at * rows, rows), :]


    def pack_stress(step):
        for d in (0, 1):
            base = NY if d else 0
            out = sent[step, YS, d]
            for at, (field, layer) in enumerate(STRESS_Y[d]):
                if step == 0:
                    value = s_in[field, pl.ds(base + layer, NX, stride=NY), :]
                else:
                    value = s_ext[field, columns(base + layer), :]
                out[pl.ds(at * NX, NX), :] = value
            if step == 0:
                for at, layer in enumerate(LIGHT[d]):
                    out[pl.ds((len(STRESS_Y[d]) + at) * NX, NX), :] = buoyancy[
                        pl.ds(base + layer, NX, stride=NY), :
                    ]
            base = NX if d else 0
            out = sent[step, XS, d]
            for at, (field, layer) in enumerate(STRESS_X[d]):
                x = base + layer
                if step == 0:
                    value = s_in[field, pl.ds(x * NY, NY), :]
                else:
                    value = s_ext[field, pl.ds((x + 2) * PITCH + NY, NY), :]
                out[pl.ds(at * NY, NY), :] = value
            if step == 0:
                for at, layer in enumerate(LIGHT[d]):
                    out[pl.ds((len(STRESS_X[d]) + at) * NY, NY), :] = buoyancy[
                        pl.ds((base + layer) * NY, NY), :
                    ]

    def pack_corner(step):
        def row(field, x, y):
            if step == 0:
                return s_in[field, pl.ds(x * NY + y, 1), :]
            return s_ext[field, pl.ds((x + 2) * PITCH + NY + y, 1), :]

        for d in ways["xy"]:
            for half, targets in enumerate(corner(d)):
                for at, (_, _, _, terms) in enumerate(targets):
                    sent[step, CORNER, d][pl.ds(half * NY + at, 1), :] = weighted(
                        [(w, row(*where)) for w, *where in terms]
                    )

    def extend(k, _):
        for j in range(TILES):
            row, base = place(k * TILES + j)
            for field in range(6):
                s_ext[field, pl.ds(pl.multiple_of(base, NY), NY), :] = s_in[
                    field, pl.ds(row, NY), :
                ]
        return _

    def move(step):
        def body(k, _):
            for j in range(TILES):
                row, base = place(k * TILES + j)
                light = (TIME_STEP / 24.0) * buoyancy[pl.ds(row, NY), :]
                main = pl.ds(pl.multiple_of(base, NY), NY)
                for c in range(3):
                    force = along_x(s_ext, *FORCE_X[c], base)
                    force += along_y(s_ext, *FORCE_Y[c], base)
                    force += along_z(s_ext, *FORCE_Z[c], base)
                    old = v_in[c, pl.ds(row, NY), :] if step == 0 else v_ext[c, main, :]
                    v_ext[c, main, :] = old + light * force
            return _

        lax.fori_loop(0, NX // TILES, body, 0)

    def mend_x(step):
        for low in (True, False):
            d = 1 if low else 0
            halo = got[step, XS, d]
            for i in (0, 1) if low else (NX - 2, NX - 1):
                light = (TIME_STEP / 24.0) * buoyancy[pl.ds(i * NY, NY), :]
                for c, (field, kind) in enumerate(FORCE_X):
                    terms = beyond(kind, low, i, NX)
                    if terms:
                        main = pl.ds((i + 2) * PITCH + NY, NY)
                        v_ext[c, main, :] += light * weighted(
                            [
                                (w, part(halo, STRESS_X[d].index((field, r)), NY))
                                for w, r in terms
                            ]
                        )

    def pack_flow_y(step):
        for d in (0, 1):
            base = NY if d else 0
            for at, (c, layer) in enumerate(FLOW_SENT_Y[d]):
                sent[step, YP, d][pl.ds(at * NX, NX), :] = v_ext[c, columns(base + layer), :]

    def mend_y(step):
        for low in (True, False):
            d = 1 if low else 0
            halo = got[step, YS, d]
            mine = sent[0, YS, 1 - d]
            for at, layer in enumerate(LIGHT[1 - d]):
                i = layer if low else NY + layer
                light = (TIME_STEP / 24.0) * part(mine, len(STRESS_Y[1 - d]) + at, NX)
                for c, (field, kind) in enumerate(FORCE_Y):
                    terms = beyond(kind, low, i, NY)
                    if terms:
                        v_ext[c, columns(i), :] += light * weighted(
                            [
                                (w, part(halo, STRESS_Y[d].index((field, r)), NX))
                                for w, r in terms
                            ]
                        )

    def pack_flow_x(step):
        for d in (0, 1):
            base = NX if d else 0
            for at, (c, layer) in enumerate(FLOW_SENT_X[d]):
                sent[step, XP, d][pl.ds(at * NY, NY), :] = v_ext[
                    c, pl.ds((base + layer + 2) * PITCH + NY, NY), :
                ]

    row_of = lax.broadcasted_iota(jnp.int32, (NY, NZ), 0)

    def scattered(step, d, half, c, layer, start):
        total = None
        for at, (field, which, i, _) in enumerate(corner(d)[half]):
            if field == c and which == layer and start <= i < start + NY:
                row = got[step, CORNER, d][pl.ds(half * NY + at, 1), :]
                rest = zero if total is None else total
                total = jnp.where(row_of == i - start, jnp.broadcast_to(row, (NY, NZ)), rest)
        return [] if total is None else [(1.0, total)]

    def finish(step, axis):
        on_y = axis == "y"
        tiles = NX // NY if on_y else 1
        rows = NX if on_y else NY
        moved, pushed = (YP, YS) if on_y else (XP, XS)
        layers_sent, pulls = (FLOW_SENT_Y, STRESS_Y) if on_y else (FLOW_SENT_X, STRESS_X)
        for low in (True, False):
            d = 1 if low else 0
            flow, first, own = got[step, moved, d], got[0, pushed, d], sent[step, pushed, 1 - d]
            for at, (c, layer) in enumerate(layers_sent[d]):
                field, kind = (FORCE_Y if on_y else FORCE_X)[c]
                for q in range(tiles):

                    def tile(ref, index):
                        return ref[pl.ds(index * rows + q * NY, NY), :]

                    terms = [
                        (WEIGHT[kind][j - layer], tile(own, pulls[1 - d].index((field, j))))
                        for j in (HIGH[kind] if low else LOW[kind])
                        if j - layer in WEIGHT[kind]
                    ]
                    for e in (0, 1):
                        way = e * 2 + d if on_y else d * 2 + e
                        terms += scattered(step, way, 0 if on_y else 1, c, layer, q * NY)
                    value = tile(flow, at)
                    if terms:
                        light = tile(first, len(pulls[d]) + LIGHT[d].index(layer))
                        value = value + (TIME_STEP / 24.0) * light * weighted(terms)
                    if on_y:
                        start = (2 + q * NY) * PITCH + NY + (layer if low else NY + layer)
                        v_ext[c, pl.ds(start, NY, stride=PITCH), :] = value
                    else:
                        x = layer if low else NX + layer
                        v_ext[c, pl.ds((x + 2) * PITCH + NY, NY), :] = value

    def stress_layer(step, x):
        row, base = place(x)
        main = pl.ds(pl.multiple_of(base, NY), NY)
        here = pl.ds(row, NY)
        mu = (TIME_STEP / 24.0) * modulus[here, :]
        lam = (TIME_STEP / 24.0) * lame[here, :]
        e_x = along_x(v_ext, 0, "B", base)
        e_y = along_y(v_ext, 1, "B", base)
        e_z = along_z(v_ext, 2, "B", base)
        dilation = lam * (e_x + e_y + e_z)
        twice = mu + mu
        rates = (
            dilation + twice * e_x,
            dilation + twice * e_y,
            dilation + twice * e_z,
            mu * (along_y(v_ext, 0, "F", base) + along_x(v_ext, 1, "F", base)),
            mu * (along_z(v_ext, 0, "F", base) + along_x(v_ext, 2, "F", base)),
            mu * (along_z(v_ext, 1, "F", base) + along_y(v_ext, 2, "F", base)),
        )
        s = [s_ext[f, main, :] + (rates[f] + inject[f, here, :]) for f in range(6)]
        pressure = (s[0] + s[1] + s[2]) * (1.0 / 3.0)
        d = [s[f] - pressure for f in range(3)]
        second = 0.5 * (d[0] * d[0] + d[1] * d[1] + d[2] * d[2])
        second = second + s[3] * s[3] + s[4] * s[4] + s[5] * s[5]
        limit = jnp.maximum(strength[here, :] - pressure * slope[here, :], 0.0)
        ratio = limit * lax.rsqrt(jnp.maximum(second, 0.0625))
        factor = jnp.where(eligible[here, :] == 1, jnp.minimum(ratio, 1.0), 1.0)
        new = [pressure + factor * d[f] for f in range(3)] + [factor * s[f] for f in (3, 4, 5)]
        for f in range(6):
            if step == STEPS - 1:
                stress_out[f, here, :] = new[f]
                if f < 3:
                    velocity_out[f, here, :] = v_ext[f, main, :]
            else:
                s_ext[f, main, :] = new[f]

    def deform(step):
        def body(k, _):
            for j in range(2):
                stress_layer(step, k * 2 + j)
            return _

        lax.fori_loop(0, NX // 2, body, 0)

    def prepare():
        total_y = size_y * NY
        origin = ((gx * NX) * total_y + gy * NY) * NZ
        within = row_of * NZ + lane

        def body(k, _):
            places = []
            for j in range(TILES):
                x = k * TILES + j
                here = pl.ds(pl.multiple_of(x * NY, NY), NY)
                which = zone[here, :]
                coh = jnp.full((NY, NZ), cohesion[0], jnp.float32)
                fri = jnp.full((NY, NZ), friction[0], jnp.float32)
                for z in range(1, 8):
                    hit = which == z
                    coh = jnp.where(hit, cohesion[z], coh)
                    fri = jnp.where(hit, friction[z], fri)
                strength[here, :] = coh * jnp.sqrt(1.0 - fri * fri)
                slope[here, :] = fri
                places.append((here, within + (origin + x * (total_y * NZ))))
            for group in ((0, 1, 2), (3, 4, 5)):
                sums = [[zero] * len(group) for _ in places]
                for source in range(16):
                    moments = [moment[f, source] for f in group]
                    for j, (here, index) in enumerate(places):
                        hit = index == cell[source]
                        for f, value in enumerate(moments):
                            sums[j][f] = sums[j][f] + jnp.where(hit, value, 0.0)
                for j, (here, index) in enumerate(places):
                    for f, field in enumerate(group):
                        inject[field, here, :] = TIME_STEP * sums[j][f]
            return _

        lax.fori_loop(0, NX // TILES, body, 0)


    for step in range(STEPS):
        for d in ways["xy"]:
            sent[step, CORNER, d][...] = jnp.zeros((2 * NY, NZ), jnp.float32)
    for load in loads[:2]:
        load.wait()
    pack_stress(0)
    pack_corner(0)
    expected = sum(t.astype(jnp.int32) for axis in ways for t in there[axis])
    expected += (PARTS - 1) * sum(c.astype(jnp.int32) for c in crosses)
    pl.semaphore_wait(barrier, expected)
    for step in range(STEPS):
        if step:
            pack_stress(step)
        send(step, YS)
        if step:
            pack_corner(step)
        send(step, CORNER)
        send(step, XS)
        if step == 0:
            lax.fori_loop(0, NX // TILES, extend, 0)
            loads[2].wait()
        move(step)
        pack_flow_y(step)
        send(step, YP)
        pack_flow_x(step)
        send(step, XP)
        if step == 0:
            for load in loads[3:]:
                load.wait()
            prepare()
        relay(step)
        receive(step, XS)
        mend_x(step)
        receive(step, XP)
        receive(step, YS)
        mend_y(step)
        receive(step, CORNER)
        finish(step, "x")
        receive(step, YP)
        finish(step, "y")
        deform(step)
    for step, kind, d in MESSAGES:

        @pl.when(there[axis_of(kind)][d])
        def _():
            remote(step, kind, d).wait_send()

    for d, p, mine in relays:

        @pl.when(mine)
        def _():
            for step, kind in PASSING:
                onward(step, kind, d, p).wait_send()


def on_device(velocity, stress, lame, modulus, buoyancy, zone, eligible, *tables):
    rows = NX * NY
    flat = [a.reshape(a.shape[:-3] + (rows, NZ)) for a in (velocity, stress, lame, modulus, buoyancy, zone, eligible)]
    f32 = jnp.float32
    hbm = pl.BlockSpec(memory_space=pl.ANY)
    buffers = [
        pltpu.VMEM((message_rows(*m), NZ), f32) for m in MESSAGES
    ]
    block = pltpu.VMEM((rows, NZ), f32)
    whole = pltpu.VMEM((rows, NZ), jnp.int32)
    v, s = pl.pallas_call(
        kernel,
        out_shape=(
            pltpu.VMEM((3, rows, NZ), f32),
            pltpu.VMEM((6, rows, NZ), f32),
        ),
        in_specs=[hbm] * 11,
        out_specs=(pl.BlockSpec(memory_space=pltpu.VMEM),) * 2,
        scratch_shapes=[
            pltpu.VMEM((6, rows, NZ), f32),
            pltpu.VMEM((3, rows, NZ), f32),
            block,
            block,
            block,
            whole,
            whole,
            pltpu.SMEM((8,), f32),
            pltpu.SMEM((8,), f32),
            pltpu.SMEM((16,), jnp.int32),
            pltpu.SMEM((6, 16), f32),
            pltpu.VMEM((6, EXT, NZ), f32),
            pltpu.VMEM((3, EXT, NZ), f32),
            block,
            block,
            pltpu.VMEM((6, rows, NZ), f32),
            *buffers,
            *buffers,
            *[pltpu.VMEM((passing_rows(*m), NZ), f32) for m in PASSING],
            pltpu.SemaphoreType.DMA((11,)),
            pltpu.SemaphoreType.DMA((len(MESSAGES),)),
            pltpu.SemaphoreType.DMA((len(MESSAGES),)),
            pltpu.SemaphoreType.DMA((max(len(PASSING), 1),)),
            pltpu.SemaphoreType.DMA((max(len(PASSING), 1),)),
        ],
        compiler_params=pltpu.CompilerParams(collective_id=0, has_side_effects=True),
    )(*flat, *tables)
    return v.reshape(velocity.shape), s.reshape(stress.shape)


def solution(mesh):
    wide, field, table = P(None, "gx", "gy", None), P("gx", "gy", None), P()
    return jax.shard_map(
        on_device,
        mesh=mesh,
        in_specs=(wide, wide) + (field,) * 5 + (table,) * 4,
        out_specs=(wide, wide),
        check_vma=False,
    )
```

```python
import functools

import jax
import jax.numpy as jnp
from jax import lax
from jax.experimental import pallas as pl
from jax.experimental.pallas import tpu as pltpu
from jax.sharding import PartitionSpec as P

STEPS = 2
TIME_STEP = 0.1
MESH = pl.DeviceIdType.MESH
NX, NY, NZ = 32, 8, 128
PITCH = 24
EXT = (NX + 4) * PITCH
TILES = 4
BENT = 4
DEEP = 16

WEIGHT = {"F": {1: 27.0, 0: -27.0, 2: -1.0, -1: 1.0}, "B": {0: 27.0, -1: -27.0, 1: -1.0, -2: 1.0}}
LOW = {"F": (-1,), "B": (-2, -1)}
HIGH = {"F": (0, 1), "B": (0,)}
FORCE_X = ((0, "F"), (3, "B"), (4, "B"))
FORCE_Y = ((3, "B"), (1, "F"), (5, "B"))
FORCE_Z = ((4, "B"), (5, "B"), (2, "F"))
FLOW_X = ((0, "B"), (1, "F"), (2, "F"))
FLOW_Y = ((0, "F"), (1, "B"), (2, "F"))
FLOW_Z = ((0, "F"), (1, "F"), (2, "B"))


def layers(table, side):
    return [(field, layer) for field, kind in table for layer in side[kind]]


STRESS_Y = (layers(FORCE_Y, HIGH), layers(FORCE_Y, LOW))
STRESS_X = (layers(FORCE_X, HIGH), layers(FORCE_X, LOW))
FLOW_SENT_Y = (layers(FLOW_Y, HIGH), layers(FLOW_Y, LOW))
FLOW_SENT_X = (layers(FLOW_X, HIGH), layers(FLOW_X, LOW))
LIGHT = ((0, 1), (-2, -1))

YS, YP, XS, XP, CORNER = range(5)
COUNTS = {
    YS: tuple(len(STRESS_Y[d]) for d in (0, 1)),
    YP: tuple(len(FLOW_SENT_Y[d]) for d in (0, 1)),
    XS: tuple(len(STRESS_X[d]) for d in (0, 1)),
    XP: tuple(len(FLOW_SENT_X[d]) for d in (0, 1)),
}


def beyond(kind, low, i, count):
    if low:
        return [(WEIGHT[kind][r - i], r) for r in LOW[kind] if r - i in WEIGHT[kind]]
    return [(WEIGHT[kind][count + r - i], r) for r in HIGH[kind] if count + r - i in WEIGHT[kind]]


def corner(direction):
    up_x, up_y = divmod(direction, 2)
    base_x, base_y = NX * up_x, NY * up_y
    along_y, along_x = [], []
    for c, layer in FLOW_SENT_Y[up_y]:
        field, kind = FORCE_X[c]
        for i in (0, 1) if up_x else (NX - 2, NX - 1):
            terms = beyond(kind, up_x, i, NX)
            if terms:
                along_y.append((c, layer, i, [(w, field, base_x + r, base_y + layer) for w, r in terms]))
    for c, layer in FLOW_SENT_X[up_x]:
        field, kind = FORCE_Y[c]
        for i in (0, 1) if up_y else (NY - 2, NY - 1):
            terms = beyond(kind, up_y, i, NY)
            if terms:
                along_x.append((c, layer, i, [(w, field, base_x + layer, base_y + r) for w, r in terms]))
    return along_y, along_x


def message_rows(step, kind, direction):
    if kind == CORNER:
        return 2 * NY
    count = COUNTS[kind][direction]
    if kind in (YS, XS) and step == 0:
        count += 2
    return count * (NX if kind in (YS, YP) else NY)


RUN = 16
SENDER = (0, RUN - 1)
RELAY = ((14, 12, 2), (1, 3, 13))
PARTS = 1 + len(RELAY[0])


def shares(step, kind, direction):
    if step == 0 and direction == 1:
        return FIRST_UP
    return LATER


FIRST_UP = (0.4, 0.34, 0.26)
LATER = (0.24, 0.24, 0.2)


def part_rows(step, kind, direction):
    rows = message_rows(step, kind, direction)
    sizes = [int(rows * share) // NY * NY for share in shares(step, kind, direction)]
    if step == 0 and direction == 1:
        sizes[0] = rows - sum(sizes[1:])
    cuts = [0, rows - sum(sizes)]
    for size in sizes:
        cuts.append(cuts[-1] + size)
    return [pl.ds(a, b - a) for a, b in zip(cuts, cuts[1:])]


MESSAGES = [
    (s, k, d) for s in range(STEPS) for k in range(5) for d in range(4 if k == CORNER else 2)
]
PASSING = [(s, k) for s in range(STEPS) for k in (YS, YP)] if PARTS > 1 else []


def passing_rows(step, kind):
    return max(r.size for d in (0, 1) for r in part_rows(step, kind, d)[1:])


def kernel(
    velocity,
    stress,
    lame_hbm,
    modulus_hbm,
    buoyancy_hbm,
    zone_hbm,
    eligible_hbm,
    cohesion_hbm,
    friction_hbm,
    cell_hbm,
    moment_hbm,
    velocity_out,
    stress_out,
    s_in,
    v_in,
    lame,
    modulus,
    buoyancy,
    zone,
    eligible,
    cohesion,
    friction,
    cell,
    moment,
    s_ext,
    v_ext,
    strength,
    slope,
    inject,
    in_depth,
    *rest,
):
    sent = dict(zip(MESSAGES, rest[: len(MESSAGES)]))
    got = dict(zip(MESSAGES, rest[len(MESSAGES) : 2 * len(MESSAGES)]))
    rest = rest[2 * len(MESSAGES) :]
    passing = dict(zip(PASSING, rest[: len(PASSING)]))
    turning = rest[len(PASSING)]
    load_sem, send_sem, recv_sem, pass_sem, onward_sem, turn_sem, turned_sem, late_sem = rest[len(PASSING) + 1 :]
    gx, gy = lax.axis_index("gx"), lax.axis_index("gy")
    size_x, size_y = lax.axis_size("gx"), lax.axis_size("gy")

    there = {"x": (gx > 0, gx < size_x - 1), "y": (gy > 0, gy < size_y - 1)}
    there["xy"] = [a & b for a in there["x"] for b in there["y"]]
    target = {
        "x": ({"gx": gx - 1}, {"gx": gx + 1}),
        "y": ({"gy": gy - 1}, {"gy": gy + 1}),
        "xy": [{"gx": gx + a, "gy": gy + b} for a in (-1, 1) for b in (-1, 1)],
    }
    ways = {"x": (0, 1), "y": (0, 1), "xy": range(4)}

    run, spot = gy // RUN, gy % RUN
    beyond_run = (run > 0, run < size_y // RUN - 1)
    crosses = [beyond_run[d] & (spot == SENDER[d]) for d in (0, 1)]
    relays = [
        (d, p, beyond_run[d] & (spot == RELAY[d][p - 1])) for d in (0, 1) for p in range(1, PARTS)
    ]

    def hub(way):
        return {"gx": gx + (1 if way // 2 else -1), "gy": run * RUN + RELAY[way % 2][0]}

    turns = [
        (way, beyond_run[way % 2] & (spot == RELAY[way % 2][0]) & there["x"][1 - way // 2])
        for way in range(4)
    ]
    aways = [there["xy"][way] & crosses[way % 2] for way in range(4)]

    origin = (gx == 0) & (gy == 0)
    beside = {
        "x": (gx == 1) & (gy == 0),
        "y": (gx == 0) & (gy == 1),
        "xy": (gx == 1) & (gy == 1),
    }
    greets, expects = {}, {}
    for axis in ways:
        last = ways[axis][-1]
        greets[axis] = [there[axis][d] & jnp.logical_not(origin) for d in ways[axis]]
        expects[axis] = list(there[axis])
        expects[axis][0] = expects[axis][0] & jnp.logical_not(beside[axis])
        if axis == "xy":
            for d in ways[axis]:
                greets[axis][d] = greets[axis][d] & jnp.logical_not(aways[d])
                expects[axis][d] = expects[axis][d] & jnp.logical_not(aways[d])
    greets["y"][0] = greets["y"][0] & jnp.logical_not(crosses[0])
    expects["y"][1] = expects["y"][1] & jnp.logical_not(crosses[1])

    barrier = pltpu.get_barrier_semaphore()

    def greet(when, where):
        @pl.when(when)
        def _():
            pl.semaphore_signal(barrier, inc=1, device_id=where, device_id_type=MESH)

    for place_up in RELAY[1]:
        greet(crosses[0], {"gy": (run - 1) * RUN + place_up})
    for d, _, mine in relays:
        greet(mine, {"gy": run * RUN + SENDER[d]})
    for way, mine in turns:
        greet(mine, {"gx": gx - (1 if way // 2 else -1), "gy": run * RUN + SENDER[way % 2]})
    for axis in ("y", "xy", "x"):
        for d in ways[axis]:
            greet(greets[axis][d], target[axis][d])

    def amount(flags):
        return sum(flag.astype(jnp.int32) for flag in flags)

    expected = amount(f for axis in ways for f in expects[axis])
    expected += (PARTS - 1) * amount(crosses) + amount(aways)
    expected += amount(mine for d, _, mine in relays if d == 1)

    loads = [
        pltpu.make_async_copy(a, b, load_sem.at[i])
        for i, (a, b) in enumerate(
            (
                (stress, s_in),
                (buoyancy_hbm, buoyancy),
                (velocity, v_in),
                (zone_hbm, zone),
                (eligible_hbm, eligible),
                (lame_hbm, lame),
                (modulus_hbm, modulus),
                (cohesion_hbm, cohesion),
                (friction_hbm, friction),
                (cell_hbm, cell),
                (moment_hbm, moment),
            )
        )
    ]
    for load in loads:
        load.start()

    def axis_of(kind):
        return {YS: "y", YP: "y", XS: "x", XP: "x", CORNER: "xy"}[kind]

    def remote(step, kind, d):
        at = MESSAGES.index((step, kind, d))
        return pltpu.make_async_remote_copy(
            src_ref=sent[step, kind, d],
            dst_ref=got[step, kind, d],
            send_sem=send_sem.at[at],
            recv_sem=recv_sem.at[at],
            device_id=target[axis_of(kind)][d],
            device_id_type=MESH,
        )

    def cut(step, kind, d, p):
        at = MESSAGES.index((step, kind, d))
        rows = part_rows(step, kind, d)[p]
        if p == 0:
            into, sem, where = got[step, kind, d].at[rows], recv_sem.at[at], target["y"][d]
        else:
            into = passing[step, kind].at[pl.ds(0, rows.size)]
            sem = pass_sem.at[PASSING.index((step, kind))]
            where = {"gy": run * RUN + RELAY[d][p - 1]}
        return pltpu.make_async_remote_copy(
            src_ref=sent[step, kind, d].at[rows],
            dst_ref=into,
            send_sem=send_sem.at[at],
            recv_sem=sem,
            device_id=where,
            device_id_type=MESH,
        )

    def onward(step, kind, d, p):
        rows = part_rows(step, kind, d)[p]
        return pltpu.make_async_remote_copy(
            src_ref=passing[step, kind].at[pl.ds(0, rows.size)],
            dst_ref=got[step, kind, d].at[rows],
            send_sem=onward_sem.at[PASSING.index((step, kind))],
            recv_sem=recv_sem.at[MESSAGES.index((step, kind, d))],
            device_id={"gy": (run + (1 if d else -1)) * RUN + SENDER[1 - d]},
            device_id_type=MESH,
        )

    def aside(step, d):
        side = d // 2
        return pltpu.make_async_remote_copy(
            src_ref=sent[step, CORNER, d],
            dst_ref=turning.at[step, side],
            send_sem=send_sem.at[MESSAGES.index((step, CORNER, d))],
            recv_sem=turn_sem.at[step, side],
            device_id=hub(d),
            device_id_type=MESH,
        )

    def turned(step, d):
        side = d // 2
        return pltpu.make_async_remote_copy(
            src_ref=turning.at[step, side],
            dst_ref=got[step, CORNER, d],
            send_sem=turned_sem.at[step, side],
            recv_sem=recv_sem.at[MESSAGES.index((step, CORNER, d))],
            device_id={"gy": (run + (1 if d % 2 else -1)) * RUN + SENDER[1 - d % 2]},
            device_id_type=MESH,
        )

    def turn(step):
        for d, mine in turns:

            @pl.when(mine)
            def _():
                aside(step, d).wait_recv()
                turned(step, d).start()

    def relay(step):
        for d, p, mine in relays:

            @pl.when(mine)
            def _():
                for kind in (YS, YP):
                    cut(step, kind, d, p).wait_recv()
                    onward(step, kind, d, p).start()

    def send(step, kind):
        axis = axis_of(kind)
        for d in ways[axis]:
            now = there[axis][d]
            if d == 0 and step == 0:
                now = now & jnp.logical_not(beside[axis])
            if axis == "x":

                @pl.when(now)
                def _():
                    remote(step, kind, d).start()

            else:
                across = aways[d] if axis == "xy" else crosses[d]

                @pl.when(now & jnp.logical_not(across))
                def _():
                    remote(step, kind, d).start()

                @pl.when(across)
                def _():
                    if axis == "xy":
                        aside(step, d).start()
                    else:
                        for p in reversed(range(PARTS)):
                            if part_rows(step, kind, d)[p].size:
                                cut(step, kind, d, p).start()

    def send_origin():
        for axis, kinds in (("y", (YS, YP)), ("xy", (CORNER,)), ("x", (XS, XP))):

            @pl.when(beside[axis])
            def _():
                pl.semaphore_wait(late_sem, 1)
                for kind in kinds:
                    remote(0, kind, 0).start()

    def receive(step, kind):
        axis = axis_of(kind)
        for d in ways[axis]:

            @pl.when(there[axis][ways[axis][-1] - d])
            def _():
                remote(step, kind, d).wait_recv()

    for axis in ways:
        for d in ways[axis]:

            @pl.when(jnp.logical_not(there[axis][ways[axis][-1] - d]))
            def _():
                for step, kind, way in MESSAGES:
                    if way == d and axis_of(kind) == axis:
                        ref = got[step, kind, way]
                        ref[...] = jnp.zeros(ref.shape, jnp.float32)

    zero = jnp.zeros((NY, NZ), jnp.float32)
    for field in (0, 3, 4):
        for x in (-2, -1, NX, NX + 1):
            s_ext[field, pl.ds((x + 2) * PITCH + NY, NY), :] = zero

    def clear(x, _):
        for field in (1, 3, 5):
            for offset in (0, 2 * NY):
                start = pl.multiple_of((x + 2) * PITCH + offset, NY)
                s_ext[field, pl.ds(start, NY), :] = zero
        return _

    lax.fori_loop(0, NX, clear, 0)

    lane = lax.broadcasted_iota(jnp.int32, (NY, NZ), 1)
    keep = {1: lane < NZ - 1, 2: lane < NZ - 2, -1: lane >= 1, -2: lane >= 2}

    def weighted(terms):
        total = None
        for weight, value in terms:
            if weight < 0 and total is not None:
                total = total - (value if weight == -1.0 else -weight * value)
            else:
                value = value if weight == 1.0 else weight * value
                total = value if total is None else total + value
        return total

    def spread(kind, at):
        if kind == "F":
            return 27.0 * (at(1) - at(0)) - (at(2) - at(-1))
        return 27.0 * (at(0) - at(-1)) - (at(1) - at(-2))

    def along_x(ref, field, kind, base):
        return spread(
            kind,
            lambda o: ref[field, pl.ds(pl.multiple_of(base + o * PITCH, NY), NY), :],
        )

    def along_y(ref, field, kind, base):
        return spread(
            kind,
            lambda o: ref[
                field, pl.ds(pl.multiple_of(base, NY) if o == 0 else base + o, NY), :
            ],
        )

    def along_z(ref, field, kind, base):
        value = ref[field, pl.ds(pl.multiple_of(base, NY), NY), :]
        return spread(kind, lambda o: turned_z(value, o))

    def turned_z(value, o):
        if o == 0:
            return value
        return jnp.where(keep[o], pltpu.roll(value, (-o) % NZ, 1), 0.0)

    def depth(ref, table):
        def body(k, _):
            for j in range(DEEP):
                row, base = place(k * DEEP + j)
                for c, (field, kind) in enumerate(table):
                    in_depth[c, pl.ds(row, NY), :] = along_z(ref, field, kind, base)
            return _

        lax.fori_loop(0, NX // DEEP, body, 0)

    def place(x):
        return pl.multiple_of(x * NY, NY), (x + 2) * PITCH + NY

    def columns(row):
        return pl.ds(2 * PITCH + NY + row, NX, stride=PITCH)

    def part(ref, at, rows):
        return ref[pl.ds(at * rows, rows), :]


    def pack_stress(step):
        for d in (0, 1):
            base = NY if d else 0
            out = sent[step, YS, d]
            for at, (field, layer) in enumerate(STRESS_Y[d]):
                if step == 0:
                    value = s_in[field, pl.ds(base + layer, NX, stride=NY), :]
                else:
                    value = s_ext[field, columns(base + layer), :]
                out[pl.ds(at * NX, NX), :] = value
            if step == 0:
                for at, layer in enumerate(LIGHT[d]):
                    out[pl.ds((len(STRESS_Y[d]) + at) * NX, NX), :] = buoyancy[
                        pl.ds(base + layer, NX, stride=NY), :
                    ]
            base = NX if d else 0
            out = sent[step, XS, d]
            for at, (field, layer) in enumerate(STRESS_X[d]):
                x = base + layer
                if step == 0:
                    value = s_in[field, pl.ds(x * NY, NY), :]
                else:
                    value = s_ext[field, pl.ds((x + 2) * PITCH + NY, NY), :]
                out[pl.ds(at * NY, NY), :] = value
            if step == 0:
                for at, layer in enumerate(LIGHT[d]):
                    out[pl.ds((len(STRESS_X[d]) + at) * NY, NY), :] = buoyancy[
                        pl.ds((base + layer) * NY, NY), :
                    ]

    def pack_corner(step):
        def row(field, x, y):
            if step == 0:
                return s_in[field, pl.ds(x * NY + y, 1), :]
            return s_ext[field, pl.ds((x + 2) * PITCH + NY + y, 1), :]

        for d in ways["xy"]:
            for half, targets in enumerate(corner(d)):
                for at, (_, _, _, terms) in enumerate(targets):
                    sent[step, CORNER, d][pl.ds(half * NY + at, 1), :] = weighted(
                        [(w, row(*where)) for w, *where in terms]
                    )

    def extend(k, _):
        for j in range(TILES):
            row, base = place(k * TILES + j)
            for field in range(6):
                s_ext[field, pl.ds(pl.multiple_of(base, NY), NY), :] = s_in[
                    field, pl.ds(row, NY), :
                ]
        return _

    def move(step):
        def body(k, _):
            for j in range(TILES):
                row, base = place(k * TILES + j)
                light = (TIME_STEP / 24.0) * buoyancy[pl.ds(row, NY), :]
                main = pl.ds(pl.multiple_of(base, NY), NY)
                for c in range(3):
                    force = along_x(s_ext, *FORCE_X[c], base)
                    force += along_y(s_ext, *FORCE_Y[c], base)
                    force += in_depth[c, pl.ds(row, NY), :]
                    old = v_in[c, pl.ds(row, NY), :] if step == 0 else v_ext[c, main, :]
                    v_ext[c, main, :] = old + light * force
            return _

        lax.fori_loop(0, NX // TILES, body, 0)

    def mend_x(step):
        for low in (True, False):
            d = 1 if low else 0
            halo = got[step, XS, d]
            for i in (0, 1) if low else (NX - 2, NX - 1):
                light = (TIME_STEP / 24.0) * buoyancy[pl.ds(i * NY, NY), :]
                for c, (field, kind) in enumerate(FORCE_X):
                    terms = beyond(kind, low, i, NX)
                    if terms:
                        main = pl.ds((i + 2) * PITCH + NY, NY)
                        v_ext[c, main, :] += light * weighted(
                            [
                                (w, part(halo, STRESS_X[d].index((field, r)), NY))
                                for w, r in terms
                            ]
                        )

    def outflow(step, c, x, y, skip):
        base = (x + 2) * PITCH + NY + y
        inner = pl.ds(x * NY + y, NY, stride=NY) if skip > 1 else pl.ds(x * NY + y, NY)

        def rows(ref, field, o):
            at = pl.ds(base + o, NY, stride=skip) if skip > 1 else pl.ds(base + o, NY)
            return ref[field, at, :]

        field, kind = FORCE_X[c]
        force = spread(kind, lambda o: rows(s_ext, field, o * PITCH))
        field, kind = FORCE_Y[c]
        force += spread(kind, lambda o: rows(s_ext, field, o))
        field, kind = FORCE_Z[c]
        value = rows(s_ext, field, 0)
        force += spread(kind, lambda o: turned_z(value, o))
        old = v_in[c, inner, :] if step == 0 else rows(v_ext, c, 0)
        return old + (TIME_STEP / 24.0) * buoyancy[inner, :] * force

    def pack_flow_y(step):
        for d in (0, 1):
            base = NY if d else 0
            for at, (c, layer) in enumerate(FLOW_SENT_Y[d]):
                for q in range(NX // NY):
                    sent[step, YP, d][pl.ds(at * NX + q * NY, NY), :] = outflow(
                        step, c, q * NY, base + layer, PITCH
                    )

    def pack_flow_x(step):
        for d in (0, 1):
            base = NX if d else 0
            for at, (c, layer) in enumerate(FLOW_SENT_X[d]):
                sent[step, XP, d][pl.ds(at * NY, NY), :] = outflow(step, c, base + layer, 0, 1)

    def mend_y(step):
        for low in (True, False):
            d = 1 if low else 0
            halo = got[step, YS, d]
            mine = sent[0, YS, 1 - d]
            for at, layer in enumerate(LIGHT[1 - d]):
                i = layer if low else NY + layer
                light = (TIME_STEP / 24.0) * part(mine, len(STRESS_Y[1 - d]) + at, NX)
                for c, (field, kind) in enumerate(FORCE_Y):
                    terms = beyond(kind, low, i, NY)
                    if terms:
                        v_ext[c, columns(i), :] += light * weighted(
                            [
                                (w, part(halo, STRESS_Y[d].index((field, r)), NX))
                                for w, r in terms
                            ]
                        )

    row_of = lax.broadcasted_iota(jnp.int32, (NY, NZ), 0)

    def scattered(step, d, half, c, layer, start):
        total = None
        for at, (field, which, i, _) in enumerate(corner(d)[half]):
            if field == c and which == layer and start <= i < start + NY:
                row = got[step, CORNER, d][pl.ds(half * NY + at, 1), :]
                rest = zero if total is None else total
                total = jnp.where(row_of == i - start, jnp.broadcast_to(row, (NY, NZ)), rest)
        return [] if total is None else [(1.0, total)]

    def finish(step, axis):
        on_y = axis == "y"
        tiles = NX // NY if on_y else 1
        rows = NX if on_y else NY
        moved, pushed = (YP, YS) if on_y else (XP, XS)
        layers_sent, pulls = (FLOW_SENT_Y, STRESS_Y) if on_y else (FLOW_SENT_X, STRESS_X)
        for low in (True, False):
            d = 1 if low else 0
            flow, first, own = got[step, moved, d], got[0, pushed, d], sent[step, pushed, 1 - d]
            for at, (c, layer) in enumerate(layers_sent[d]):
                field, kind = (FORCE_Y if on_y else FORCE_X)[c]
                for q in range(tiles):

                    def tile(ref, index):
                        return ref[pl.ds(index * rows + q * NY, NY), :]

                    terms = [
                        (WEIGHT[kind][j - layer], tile(own, pulls[1 - d].index((field, j))))
                        for j in (HIGH[kind] if low else LOW[kind])
                        if j - layer in WEIGHT[kind]
                    ]
                    for e in (0, 1):
                        way = e * 2 + d if on_y else d * 2 + e
                        terms += scattered(step, way, 0 if on_y else 1, c, layer, q * NY)
                    value = tile(flow, at)
                    if terms:
                        light = tile(first, len(pulls[d]) + LIGHT[d].index(layer))
                        value = value + (TIME_STEP / 24.0) * light * weighted(terms)
                    if on_y:
                        start = (2 + q * NY) * PITCH + NY + (layer if low else NY + layer)
                        v_ext[c, pl.ds(start, NY, stride=PITCH), :] = value
                    else:
                        x = layer if low else NX + layer
                        v_ext[c, pl.ds((x + 2) * PITCH + NY, NY), :] = value

    def stress_layer(step, x):
        row, base = place(x)
        main = pl.ds(pl.multiple_of(base, NY), NY)
        here = pl.ds(row, NY)
        mu = (TIME_STEP / 24.0) * modulus[here, :]
        lam = (TIME_STEP / 24.0) * lame[here, :]
        e_x = along_x(v_ext, 0, "B", base)
        e_y = along_y(v_ext, 1, "B", base)
        e_z = in_depth[2, here, :]
        dilation = lam * (e_x + e_y + e_z)
        twice = mu + mu
        rates = (
            dilation + twice * e_x,
            dilation + twice * e_y,
            dilation + twice * e_z,
            mu * (along_y(v_ext, 0, "F", base) + along_x(v_ext, 1, "F", base)),
            mu * (in_depth[0, here, :] + along_x(v_ext, 2, "F", base)),
            mu * (in_depth[1, here, :] + along_y(v_ext, 2, "F", base)),
        )
        s = [s_ext[f, main, :] + (rates[f] + inject[f, here, :]) for f in range(6)]
        pressure = (s[0] + s[1] + s[2]) * (1.0 / 3.0)
        d = [s[f] - pressure for f in range(3)]
        second = 0.5 * (d[0] * d[0] + d[1] * d[1] + d[2] * d[2])
        second = second + s[3] * s[3] + s[4] * s[4] + s[5] * s[5]
        limit = jnp.maximum(strength[here, :] - pressure * slope[here, :], 0.0)
        ratio = limit * lax.rsqrt(jnp.maximum(second, 0.0625))
        factor = jnp.where(eligible[here, :] == 1, jnp.minimum(ratio, 1.0), 1.0)
        new = [pressure + factor * d[f] for f in range(3)] + [factor * s[f] for f in (3, 4, 5)]
        for f in range(6):
            if step == STEPS - 1:
                stress_out[f, here, :] = new[f]
                if f < 3:
                    velocity_out[f, here, :] = v_ext[f, main, :]
            else:
                s_ext[f, main, :] = new[f]

    def deform(step):
        def body(k, _):
            for j in range(BENT):
                stress_layer(step, k * BENT + j)
            return _

        lax.fori_loop(0, NX // BENT, body, 0)

    def prepare():
        total_y = size_y * NY
        first = ((gx * NX) * total_y + gy * NY) * NZ
        within = row_of * NZ + lane

        def body(k, _):
            places = []
            for j in range(TILES):
                x = k * TILES + j
                here = pl.ds(pl.multiple_of(x * NY, NY), NY)
                which = zone[here, :]
                coh = jnp.full((NY, NZ), cohesion[0], jnp.float32)
                fri = jnp.full((NY, NZ), friction[0], jnp.float32)
                for z in range(1, 8):
                    hit = which == z
                    coh = jnp.where(hit, cohesion[z], coh)
                    fri = jnp.where(hit, friction[z], fri)
                strength[here, :] = coh * jnp.sqrt(1.0 - fri * fri)
                slope[here, :] = fri
                places.append((here, within + (first + x * (total_y * NZ))))
            for group in ((0, 1, 2), (3, 4, 5)):
                sums = [[zero] * len(group) for _ in places]
                for source in range(16):
                    moments = [moment[f, source] for f in group]
                    for j, (here, index) in enumerate(places):
                        hit = index == cell[source]
                        for f, value in enumerate(moments):
                            sums[j][f] = sums[j][f] + jnp.where(hit, value, 0.0)
                for j, (here, index) in enumerate(places):
                    for f, field in enumerate(group):
                        inject[field, here, :] = TIME_STEP * sums[j][f]
            return _

        lax.fori_loop(0, NX // TILES, body, 0)


    for step in range(STEPS):
        for d in ways["xy"]:
            sent[step, CORNER, d][...] = jnp.zeros((2 * NY, NZ), jnp.float32)
    for step in range(STEPS):
        if step == 0:
            for load in loads[:2]:
                load.wait()
            lax.fori_loop(0, NX // TILES, extend, 0)
            loads[2].wait()
        pack_stress(step)
        if step == 0:
            pack_corner(step)
            pack_flow_y(step)
            pack_flow_x(step)
            pl.semaphore_wait(barrier, expected)
            for axis in ways:
                up = ways[axis][-1]

                @pl.when(origin & there[axis][up])
                def _():
                    pl.semaphore_signal(
                        late_sem, inc=1, device_id=target[axis][up], device_id_type=MESH
                    )

        send(step, YS)
        if step:
            pack_corner(step)
        send(step, CORNER)
        send(step, XS)
        if step:
            pack_flow_y(step)
        send(step, YP)
        if step:
            pack_flow_x(step)
        send(step, XP)
        if step == 0:
            relay(step)
            turn(step)
        depth(s_ext, FORCE_Z)
        move(step)
        if step == 0:
            for load in loads[3:]:
                load.wait()
            prepare()
            send_origin()
        else:
            relay(step)
            turn(step)
        receive(step, XS)
        mend_x(step)
        receive(step, XP)
        receive(step, YS)
        mend_y(step)
        depth(v_ext, FLOW_Z)
        receive(step, CORNER)
        finish(step, "x")
        receive(step, YP)
        finish(step, "y")
        deform(step)
    for step, kind, d in MESSAGES:

        @pl.when(there[axis_of(kind)][d])
        def _():
            remote(step, kind, d).wait_send()

    for d, mine in turns:

        @pl.when(mine)
        def _():
            for step in range(STEPS):
                turned(step, d).wait_send()

    for d, p, mine in relays:

        @pl.when(mine)
        def _():
            for step, kind in PASSING:
                onward(step, kind, d, p).wait_send()


def write(velocity, stress, velocity_out, stress_out, sem):
    copies = [
        pltpu.make_async_copy(a.at[f], b.at[f], sem.at[at])
        for at, (a, b, f) in enumerate(
            [(velocity, velocity_out, f) for f in range(3)] + [(stress, stress_out, f) for f in range(6)]
        )
    ]
    for copy in copies:
        copy.start()
    for copy in copies:
        copy.wait()


def on_device(velocity, stress, lame, modulus, buoyancy, zone, eligible, *tables):
    rows = NX * NY
    flat = [a.reshape(a.shape[:-3] + (rows, NZ)) for a in (velocity, stress, lame, modulus, buoyancy, zone, eligible)]
    f32 = jnp.float32
    hbm = pl.BlockSpec(memory_space=pl.ANY)
    buffers = [
        pltpu.VMEM((message_rows(*m), NZ), f32) for m in MESSAGES
    ]
    block = pltpu.VMEM((rows, NZ), f32)
    whole = pltpu.VMEM((rows, NZ), jnp.int32)
    v, s = pl.pallas_call(
        kernel,
        out_shape=(
            pltpu.VMEM((3, rows, NZ), f32),
            pltpu.VMEM((6, rows, NZ), f32),
        ),
        in_specs=[hbm] * 11,
        out_specs=(pl.BlockSpec(memory_space=pltpu.VMEM),) * 2,
        scratch_shapes=[
            pltpu.VMEM((6, rows, NZ), f32),
            pltpu.VMEM((3, rows, NZ), f32),
            block,
            block,
            block,
            whole,
            whole,
            pltpu.SMEM((8,), f32),
            pltpu.SMEM((8,), f32),
            pltpu.SMEM((16,), jnp.int32),
            pltpu.SMEM((6, 16), f32),
            pltpu.VMEM((6, EXT, NZ), f32),
            pltpu.VMEM((3, EXT, NZ), f32),
            block,
            block,
            pltpu.VMEM((6, rows, NZ), f32),
            pltpu.VMEM((3, rows, NZ), f32),
            *buffers,
            *buffers,
            *[pltpu.VMEM((passing_rows(*m), NZ), f32) for m in PASSING],
            pltpu.VMEM((STEPS, 2, 2 * NY, NZ), f32),
            pltpu.SemaphoreType.DMA((11,)),
            pltpu.SemaphoreType.DMA((len(MESSAGES),)),
            pltpu.SemaphoreType.DMA((len(MESSAGES),)),
            pltpu.SemaphoreType.DMA((max(len(PASSING), 1),)),
            pltpu.SemaphoreType.DMA((max(len(PASSING), 1),)),
            pltpu.SemaphoreType.DMA((STEPS, 2)),
            pltpu.SemaphoreType.DMA((STEPS, 2)),
            pltpu.SemaphoreType.REGULAR,
        ],
        compiler_params=pltpu.CompilerParams(collective_id=0, has_side_effects=True),
    )(*flat, *tables)
    v, s = pl.pallas_call(
        write,
        out_shape=(
            jax.ShapeDtypeStruct((3, rows, NZ), f32),
            jax.ShapeDtypeStruct((6, rows, NZ), f32),
        ),
        in_specs=[hbm] * 2,
        out_specs=(hbm, hbm),
        scratch_shapes=[pltpu.SemaphoreType.DMA((9,))],
        compiler_params=pltpu.CompilerParams(vmem_limit_bytes=1 << 20),
    )(v, s)
    return v.reshape(velocity.shape), s.reshape(stress.shape)


def solution(mesh):
    wide, field, table = P(None, "gx", "gy", None), P("gx", "gy", None), P()
    return jax.shard_map(
        on_device,
        mesh=mesh,
        in_specs=(wide, wide) + (field,) * 5 + (table,) * 4,
        out_specs=(wide, wide),
        check_vma=False,
    )
```

```python
import functools

import jax
import jax.numpy as jnp
from jax import lax
from jax.experimental import pallas as pl
from jax.experimental.pallas import tpu as pltpu
from jax.sharding import PartitionSpec as P

STEPS = 2
TIME_STEP = 0.1
MESH = pl.DeviceIdType.MESH
NX, NY, NZ = 32, 8, 128
PITCH = 24
EXT = (NX + 4) * PITCH
TILES = 4
BENT = 4
DEEP = 16

WEIGHT = {"F": {1: 27.0, 0: -27.0, 2: -1.0, -1: 1.0}, "B": {0: 27.0, -1: -27.0, 1: -1.0, -2: 1.0}}
LOW = {"F": (-1,), "B": (-2, -1)}
HIGH = {"F": (0, 1), "B": (0,)}
FORCE_X = ((0, "F"), (3, "B"), (4, "B"))
FORCE_Y = ((3, "B"), (1, "F"), (5, "B"))
FORCE_Z = ((4, "B"), (5, "B"), (2, "F"))
FLOW_X = ((0, "B"), (1, "F"), (2, "F"))
FLOW_Y = ((0, "F"), (1, "B"), (2, "F"))
FLOW_Z = ((0, "F"), (1, "F"), (2, "B"))


def layers(table, side):
    return [(field, layer) for field, kind in table for layer in side[kind]]


STRESS_Y = (layers(FORCE_Y, HIGH), layers(FORCE_Y, LOW))
STRESS_X = (layers(FORCE_X, HIGH), layers(FORCE_X, LOW))
FLOW_SENT_Y = (layers(FLOW_Y, HIGH), layers(FLOW_Y, LOW))
FLOW_SENT_X = (layers(FLOW_X, HIGH), layers(FLOW_X, LOW))
LIGHT = ((0, 1), (-2, -1))

YS, YP, XS, XP, CORNER = range(5)
COUNTS = {
    YS: tuple(len(STRESS_Y[d]) for d in (0, 1)),
    YP: tuple(len(FLOW_SENT_Y[d]) for d in (0, 1)),
    XS: tuple(len(STRESS_X[d]) for d in (0, 1)),
    XP: tuple(len(FLOW_SENT_X[d]) for d in (0, 1)),
}


def beyond(kind, low, i, count):
    if low:
        return [(WEIGHT[kind][r - i], r) for r in LOW[kind] if r - i in WEIGHT[kind]]
    return [(WEIGHT[kind][count + r - i], r) for r in HIGH[kind] if count + r - i in WEIGHT[kind]]


def corner(direction):
    up_x, up_y = divmod(direction, 2)
    base_x, base_y = NX * up_x, NY * up_y
    along_y, along_x = [], []
    for c, layer in FLOW_SENT_Y[up_y]:
        field, kind = FORCE_X[c]
        for i in (0, 1) if up_x else (NX - 2, NX - 1):
            terms = beyond(kind, up_x, i, NX)
            if terms:
                along_y.append((c, layer, i, [(w, field, base_x + r, base_y + layer) for w, r in terms]))
    for c, layer in FLOW_SENT_X[up_x]:
        field, kind = FORCE_Y[c]
        for i in (0, 1) if up_y else (NY - 2, NY - 1):
            terms = beyond(kind, up_y, i, NY)
            if terms:
                along_x.append((c, layer, i, [(w, field, base_x + layer, base_y + r) for w, r in terms]))
    return along_y, along_x


def message_rows(step, kind, direction):
    if kind == CORNER:
        return 2 * NY
    count = COUNTS[kind][direction]
    if kind in (YS, XS) and step == 0:
        count += 2
    return count * (NX if kind in (YS, YP) else NY)


RUN = 16
SENDER = (0, RUN - 1)
RELAY = ((14, 12, 2), (1, 3, 13))
PARTS = 1 + len(RELAY[0])


def shares(step, kind, direction):
    if step == 0 and direction == 1:
        return FIRST_UP
    return LATER


FIRST_UP = (0.4, 0.34, 0.26)
LATER = (0.24, 0.24, 0.2)


def part_rows(step, kind, direction):
    rows = message_rows(step, kind, direction)
    sizes = [int(rows * share) // NY * NY for share in shares(step, kind, direction)]
    if step == 0 and direction == 1:
        sizes[0] = rows - sum(sizes[1:])
    cuts = [0, rows - sum(sizes)]
    for size in sizes:
        cuts.append(cuts[-1] + size)
    return [pl.ds(a, b - a) for a, b in zip(cuts, cuts[1:])]


MESSAGES = [
    (s, k, d) for s in range(STEPS) for k in range(5) for d in range(4 if k == CORNER else 2)
]
PASSING = [(s, k) for s in range(STEPS) for k in (YS, YP)] if PARTS > 1 else []


def passing_rows(step, kind):
    return max(r.size for d in (0, 1) for r in part_rows(step, kind, d)[1:])


def kernel(
    velocity,
    stress,
    lame_hbm,
    modulus_hbm,
    buoyancy_hbm,
    zone_hbm,
    eligible_hbm,
    cohesion_hbm,
    friction_hbm,
    cell_hbm,
    moment_hbm,
    velocity_out,
    stress_out,
    s_in,
    v_in,
    lame,
    modulus,
    buoyancy,
    zone,
    eligible,
    cohesion,
    friction,
    cell,
    moment,
    s_ext,
    v_ext,
    strength,
    slope,
    inject,
    in_depth,
    *rest,
):
    sent = dict(zip(MESSAGES, rest[: len(MESSAGES)]))
    got = dict(zip(MESSAGES, rest[len(MESSAGES) : 2 * len(MESSAGES)]))
    rest = rest[2 * len(MESSAGES) :]
    passing = dict(zip(PASSING, rest[: len(PASSING)]))
    turning = rest[len(PASSING)]
    load_sem, send_sem, recv_sem, pass_sem, onward_sem, turn_sem, turned_sem, late_sem = rest[len(PASSING) + 1 :]
    gx, gy = lax.axis_index("gx"), lax.axis_index("gy")
    size_x, size_y = lax.axis_size("gx"), lax.axis_size("gy")

    there = {"x": (gx > 0, gx < size_x - 1), "y": (gy > 0, gy < size_y - 1)}
    there["xy"] = [a & b for a in there["x"] for b in there["y"]]
    target = {
        "x": ({"gx": gx - 1}, {"gx": gx + 1}),
        "y": ({"gy": gy - 1}, {"gy": gy + 1}),
        "xy": [{"gx": gx + a, "gy": gy + b} for a in (-1, 1) for b in (-1, 1)],
    }
    ways = {"x": (0, 1), "y": (0, 1), "xy": range(4)}

    run, spot = gy // RUN, gy % RUN
    beyond_run = (run > 0, run < size_y // RUN - 1)
    crosses = [beyond_run[d] & (spot == SENDER[d]) for d in (0, 1)]
    relays = [
        (d, p, beyond_run[d] & (spot == RELAY[d][p - 1])) for d in (0, 1) for p in range(1, PARTS)
    ]

    def hub(way):
        return {"gx": gx + (1 if way // 2 else -1), "gy": run * RUN + RELAY[way % 2][0]}

    turns = [
        (way, beyond_run[way % 2] & (spot == RELAY[way % 2][0]) & there["x"][1 - way // 2])
        for way in range(4)
    ]
    aways = [there["xy"][way] & crosses[way % 2] for way in range(4)]

    origin = (gx == 0) & (gy == 0)
    beside = {
        "x": (gx == 1) & (gy == 0),
        "y": (gx == 0) & (gy == 1),
        "xy": (gx == 1) & (gy == 1),
    }
    greets, expects = {}, {}
    for axis in ways:
        last = ways[axis][-1]
        greets[axis] = [there[axis][d] & jnp.logical_not(origin) for d in ways[axis]]
        expects[axis] = list(there[axis])
        expects[axis][0] = expects[axis][0] & jnp.logical_not(beside[axis])
        if axis == "xy":
            for d in ways[axis]:
                greets[axis][d] = greets[axis][d] & jnp.logical_not(aways[d])
                expects[axis][d] = expects[axis][d] & jnp.logical_not(aways[d])
    greets["y"][0] = greets["y"][0] & jnp.logical_not(crosses[0])
    expects["y"][1] = expects["y"][1] & jnp.logical_not(crosses[1])

    barrier = pltpu.get_barrier_semaphore()

    def greet(when, where):
        @pl.when(when)
        def _():
            pl.semaphore_signal(barrier, inc=1, device_id=where, device_id_type=MESH)

    for place_up in RELAY[1]:
        greet(crosses[0], {"gy": (run - 1) * RUN + place_up})
    for d, _, mine in relays:
        greet(mine, {"gy": run * RUN + SENDER[d]})
    for way, mine in turns:
        greet(mine, {"gx": gx - (1 if way // 2 else -1), "gy": run * RUN + SENDER[way % 2]})
    for axis in ("y", "xy", "x"):
        for d in ways[axis]:
            greet(greets[axis][d], target[axis][d])

    def amount(flags):
        return sum(flag.astype(jnp.int32) for flag in flags)

    expected = amount(f for axis in ways for f in expects[axis])
    expected += (PARTS - 1) * amount(crosses) + amount(aways)
    expected += amount(mine for d, _, mine in relays if d == 1)

    loads = [
        pltpu.make_async_copy(a, b, load_sem.at[i])
        for i, (a, b) in enumerate(
            (
                (stress, s_in),
                (buoyancy_hbm, buoyancy),
                (velocity, v_in),
                (zone_hbm, zone),
                (eligible_hbm, eligible),
                (lame_hbm, lame),
                (modulus_hbm, modulus),
                (cohesion_hbm, cohesion),
                (friction_hbm, friction),
                (cell_hbm, cell),
                (moment_hbm, moment),
            )
        )
    ]
    for load in loads:
        load.start()

    def axis_of(kind):
        return {YS: "y", YP: "y", XS: "x", XP: "x", CORNER: "xy"}[kind]

    def remote(step, kind, d):
        at = MESSAGES.index((step, kind, d))
        return pltpu.make_async_remote_copy(
            src_ref=sent[step, kind, d],
            dst_ref=got[step, kind, d],
            send_sem=send_sem.at[at],
            recv_sem=recv_sem.at[at],
            device_id=target[axis_of(kind)][d],
            device_id_type=MESH,
        )

    def cut(step, kind, d, p):
        at = MESSAGES.index((step, kind, d))
        rows = part_rows(step, kind, d)[p]
        if p == 0:
            into, sem, where = got[step, kind, d].at[rows], recv_sem.at[at], target["y"][d]
        else:
            into = passing[step, kind].at[pl.ds(0, rows.size)]
            sem = pass_sem.at[PASSING.index((step, kind))]
            where = {"gy": run * RUN + RELAY[d][p - 1]}
        return pltpu.make_async_remote_copy(
            src_ref=sent[step, kind, d].at[rows],
            dst_ref=into,
            send_sem=send_sem.at[at],
            recv_sem=sem,
            device_id=where,
            device_id_type=MESH,
        )

    def onward(step, kind, d, p):
        rows = part_rows(step, kind, d)[p]
        return pltpu.make_async_remote_copy(
            src_ref=passing[step, kind].at[pl.ds(0, rows.size)],
            dst_ref=got[step, kind, d].at[rows],
            send_sem=onward_sem.at[PASSING.index((step, kind))],
            recv_sem=recv_sem.at[MESSAGES.index((step, kind, d))],
            device_id={"gy": (run + (1 if d else -1)) * RUN + SENDER[1 - d]},
            device_id_type=MESH,
        )

    def aside(step, d):
        side = d // 2
        return pltpu.make_async_remote_copy(
            src_ref=sent[step, CORNER, d],
            dst_ref=turning.at[step, side],
            send_sem=send_sem.at[MESSAGES.index((step, CORNER, d))],
            recv_sem=turn_sem.at[step, side],
            device_id=hub(d),
            device_id_type=MESH,
        )

    def turned(step, d):
        side = d // 2
        return pltpu.make_async_remote_copy(
            src_ref=turning.at[step, side],
            dst_ref=got[step, CORNER, d],
            send_sem=turned_sem.at[step, side],
            recv_sem=recv_sem.at[MESSAGES.index((step, CORNER, d))],
            device_id={"gy": (run + (1 if d % 2 else -1)) * RUN + SENDER[1 - d % 2]},
            device_id_type=MESH,
        )

    def turn(step):
        for d, mine in turns:

            @pl.when(mine)
            def _():
                aside(step, d).wait_recv()
                turned(step, d).start()

    def relay(step):
        for d, p, mine in relays:

            @pl.when(mine)
            def _():
                for kind in (YS, YP):
                    cut(step, kind, d, p).wait_recv()
                    onward(step, kind, d, p).start()

    def send(step, kind):
        axis = axis_of(kind)
        for d in ways[axis]:
            now = there[axis][d]
            if d == 0 and step == 0:
                now = now & jnp.logical_not(beside[axis])
            if axis == "x":

                @pl.when(now)
                def _():
                    remote(step, kind, d).start()

            else:
                across = aways[d] if axis == "xy" else crosses[d]

                @pl.when(now & jnp.logical_not(across))
                def _():
                    remote(step, kind, d).start()

                @pl.when(across)
                def _():
                    if axis == "xy":
                        aside(step, d).start()
                    else:
                        for p in reversed(range(PARTS)):
                            if part_rows(step, kind, d)[p].size:
                                cut(step, kind, d, p).start()

    def send_origin():
        for axis, kinds in (("y", (YS, YP)), ("xy", (CORNER,)), ("x", (XS, XP))):

            @pl.when(beside[axis])
            def _():
                pl.semaphore_wait(late_sem, 1)
                for kind in kinds:
                    remote(0, kind, 0).start()

    def receive(step, kind):
        axis = axis_of(kind)
        for d in ways[axis]:

            @pl.when(there[axis][ways[axis][-1] - d])
            def _():
                remote(step, kind, d).wait_recv()

    for axis in ways:
        for d in ways[axis]:

            @pl.when(jnp.logical_not(there[axis][ways[axis][-1] - d]))
            def _():
                for step, kind, way in MESSAGES:
                    if way == d and axis_of(kind) == axis:
                        ref = got[step, kind, way]
                        ref[...] = jnp.zeros(ref.shape, jnp.float32)

    zero = jnp.zeros((NY, NZ), jnp.float32)
    for field in (0, 3, 4):
        for x in (-2, -1, NX, NX + 1):
            s_ext[field, pl.ds((x + 2) * PITCH + NY, NY), :] = zero

    def clear(x, _):
        for field in (1, 3, 5):
            for offset in (0, 2 * NY):
                start = pl.multiple_of((x + 2) * PITCH + offset, NY)
                s_ext[field, pl.ds(start, NY), :] = zero
        return _

    lax.fori_loop(0, NX, clear, 0)

    lane = lax.broadcasted_iota(jnp.int32, (NY, NZ), 1)

    def keep(o, rows):
        at = lax.broadcasted_iota(jnp.int32, (rows, NZ), 1)
        return at < NZ - o if o > 0 else at >= -o


    def weighted(terms):
        total = None
        for weight, value in terms:
            if weight < 0 and total is not None:
                total = total - (value if weight == -1.0 else -weight * value)
            else:
                value = value if weight == 1.0 else weight * value
                total = value if total is None else total + value
        return total

    def spread(kind, at):
        if kind == "F":
            return 27.0 * (at(1) - at(0)) - (at(2) - at(-1))
        return 27.0 * (at(0) - at(-1)) - (at(1) - at(-2))

    def along_x(ref, field, kind, base):
        return spread(
            kind,
            lambda o: ref[field, pl.ds(pl.multiple_of(base + o * PITCH, NY), NY), :],
        )

    def along_y(ref, field, kind, base):
        return spread(
            kind,
            lambda o: ref[
                field, pl.ds(pl.multiple_of(base, NY) if o == 0 else base + o, NY), :
            ],
        )

    def along_z(ref, field, kind, base):
        value = ref[field, pl.ds(pl.multiple_of(base, NY), NY), :]
        return spread(kind, lambda o: turned_z(value, o))

    def turned_z(value, o):
        if o == 0:
            return value
        return jnp.where(keep(o, value.shape[0]), pltpu.roll(value, (-o) % NZ, 1), 0.0)

    def depth(ref, table):
        def body(k, _):
            for j in range(DEEP):
                row, base = place(k * DEEP + j)
                for c, (field, kind) in enumerate(table):
                    in_depth[c, pl.ds(row, NY), :] = along_z(ref, field, kind, base)
            return _

        lax.fori_loop(0, NX // DEEP, body, 0)

    def place(x):
        return pl.multiple_of(x * NY, NY), (x + 2) * PITCH + NY

    def columns(row):
        return pl.ds(2 * PITCH + NY + row, NX, stride=PITCH)

    def part(ref, at, rows):
        return ref[pl.ds(at * rows, rows), :]


    def pack_stress(step):
        for d in (0, 1):
            base = NY if d else 0
            out = sent[step, YS, d]
            for at, (field, layer) in enumerate(STRESS_Y[d]):
                if step == 0:
                    value = s_in[field, pl.ds(base + layer, NX, stride=NY), :]
                else:
                    value = s_ext[field, columns(base + layer), :]
                out[pl.ds(at * NX, NX), :] = value
            if step == 0:
                for at, layer in enumerate(LIGHT[d]):
                    out[pl.ds((len(STRESS_Y[d]) + at) * NX, NX), :] = buoyancy[
                        pl.ds(base + layer, NX, stride=NY), :
                    ]
            base = NX if d else 0
            out = sent[step, XS, d]
            for at, (field, layer) in enumerate(STRESS_X[d]):
                x = base + layer
                if step == 0:
                    value = s_in[field, pl.ds(x * NY, NY), :]
                else:
                    value = s_ext[field, pl.ds((x + 2) * PITCH + NY, NY), :]
                out[pl.ds(at * NY, NY), :] = value
            if step == 0:
                for at, layer in enumerate(LIGHT[d]):
                    out[pl.ds((len(STRESS_X[d]) + at) * NY, NY), :] = buoyancy[
                        pl.ds((base + layer) * NY, NY), :
                    ]

    def pack_corner(step):
        def row(field, x, y):
            if step == 0:
                return s_in[field, pl.ds(x * NY + y, 1), :]
            return s_ext[field, pl.ds((x + 2) * PITCH + NY + y, 1), :]

        for d in ways["xy"]:
            for half, targets in enumerate(corner(d)):
                for at, (_, _, _, terms) in enumerate(targets):
                    sent[step, CORNER, d][pl.ds(half * NY + at, 1), :] = weighted(
                        [(w, row(*where)) for w, *where in terms]
                    )

    def extend(k, _):
        for j in range(TILES):
            row, base = place(k * TILES + j)
            for field in range(6):
                s_ext[field, pl.ds(pl.multiple_of(base, NY), NY), :] = s_in[
                    field, pl.ds(row, NY), :
                ]
        return _

    def move(step):
        def body(k, _):
            for j in range(TILES):
                row, base = place(k * TILES + j)
                light = (TIME_STEP / 24.0) * buoyancy[pl.ds(row, NY), :]
                main = pl.ds(pl.multiple_of(base, NY), NY)
                for c in range(3):
                    force = along_x(s_ext, *FORCE_X[c], base)
                    force += along_y(s_ext, *FORCE_Y[c], base)
                    force += in_depth[c, pl.ds(row, NY), :]
                    old = v_in[c, pl.ds(row, NY), :] if step == 0 else v_ext[c, main, :]
                    v_ext[c, main, :] = old + light * force
            return _

        lax.fori_loop(0, NX // TILES, body, 0)

    def mend_x(step):
        for low in (True, False):
            d = 1 if low else 0
            halo = got[step, XS, d]
            for i in (0, 1) if low else (NX - 2, NX - 1):
                light = (TIME_STEP / 24.0) * buoyancy[pl.ds(i * NY, NY), :]
                for c, (field, kind) in enumerate(FORCE_X):
                    terms = beyond(kind, low, i, NX)
                    if terms:
                        main = pl.ds((i + 2) * PITCH + NY, NY)
                        v_ext[c, main, :] += light * weighted(
                            [
                                (w, part(halo, STRESS_X[d].index((field, r)), NY))
                                for w, r in terms
                            ]
                        )

    def outflow(step, c, x, y, skip):
        base = (x + 2) * PITCH + NY + y
        inner = pl.ds(x * NY + y, NY, stride=NY) if skip > 1 else pl.ds(x * NY + y, NY)

        def rows(ref, field, o):
            at = pl.ds(base + o, NY, stride=skip) if skip > 1 else pl.ds(base + o, NY)
            return ref[field, at, :]

        field, kind = FORCE_X[c]
        force = spread(kind, lambda o: rows(s_ext, field, o * PITCH))
        field, kind = FORCE_Y[c]
        force += spread(kind, lambda o: rows(s_ext, field, o))
        field, kind = FORCE_Z[c]
        value = rows(s_ext, field, 0)
        force += spread(kind, lambda o: turned_z(value, o))
        old = v_in[c, inner, :] if step == 0 else rows(v_ext, c, 0)
        return old + (TIME_STEP / 24.0) * buoyancy[inner, :] * force

    def pack_flow_y(step):
        for d in (0, 1):
            base = NY if d else 0
            for at, (c, layer) in enumerate(FLOW_SENT_Y[d]):
                for q in range(NX // NY):
                    sent[step, YP, d][pl.ds(at * NX + q * NY, NY), :] = outflow(
                        step, c, q * NY, base + layer, PITCH
                    )

    def pack_flow_x(step):
        for d in (0, 1):
            base = NX if d else 0
            for at, (c, layer) in enumerate(FLOW_SENT_X[d]):
                sent[step, XP, d][pl.ds(at * NY, NY), :] = outflow(step, c, base + layer, 0, 1)

    def mend_y(step):
        for low in (True, False):
            d = 1 if low else 0
            halo = got[step, YS, d]
            mine = sent[0, YS, 1 - d]
            for at, layer in enumerate(LIGHT[1 - d]):
                i = layer if low else NY + layer
                light = (TIME_STEP / 24.0) * part(mine, len(STRESS_Y[1 - d]) + at, NX)
                for c, (field, kind) in enumerate(FORCE_Y):
                    terms = beyond(kind, low, i, NY)
                    if terms:
                        value = v_ext[c, columns(i), :] + light * weighted(
                            [
                                (w, part(halo, STRESS_Y[d].index((field, r)), NX))
                                for w, r in terms
                            ]
                        )
                        v_ext[c, columns(i), :] = value
                        in_depth[c, pl.ds(i, NX, stride=NY), :] = spread(
                            FLOW_Z[c][1], lambda o: turned_z(value, o)
                        )

    row_of = lax.broadcasted_iota(jnp.int32, (NY, NZ), 0)

    def scattered(step, d, half, c, layer, start):
        total = None
        for at, (field, which, i, _) in enumerate(corner(d)[half]):
            if field == c and which == layer and start <= i < start + NY:
                row = got[step, CORNER, d][pl.ds(half * NY + at, 1), :]
                rest = zero if total is None else total
                total = jnp.where(row_of == i - start, jnp.broadcast_to(row, (NY, NZ)), rest)
        return [] if total is None else [(1.0, total)]

    def finish(step, axis):
        on_y = axis == "y"
        tiles = NX // NY if on_y else 1
        rows = NX if on_y else NY
        moved, pushed = (YP, YS) if on_y else (XP, XS)
        layers_sent, pulls = (FLOW_SENT_Y, STRESS_Y) if on_y else (FLOW_SENT_X, STRESS_X)
        for low in (True, False):
            d = 1 if low else 0
            flow, first, own = got[step, moved, d], got[0, pushed, d], sent[step, pushed, 1 - d]
            for at, (c, layer) in enumerate(layers_sent[d]):
                field, kind = (FORCE_Y if on_y else FORCE_X)[c]
                for q in range(tiles):

                    def tile(ref, index):
                        return ref[pl.ds(index * rows + q * NY, NY), :]

                    terms = [
                        (WEIGHT[kind][j - layer], tile(own, pulls[1 - d].index((field, j))))
                        for j in (HIGH[kind] if low else LOW[kind])
                        if j - layer in WEIGHT[kind]
                    ]
                    for e in (0, 1):
                        way = e * 2 + d if on_y else d * 2 + e
                        terms += scattered(step, way, 0 if on_y else 1, c, layer, q * NY)
                    value = tile(flow, at)
                    if terms:
                        light = tile(first, len(pulls[d]) + LIGHT[d].index(layer))
                        value = value + (TIME_STEP / 24.0) * light * weighted(terms)
                    if on_y:
                        start = (2 + q * NY) * PITCH + NY + (layer if low else NY + layer)
                        v_ext[c, pl.ds(start, NY, stride=PITCH), :] = value
                    else:
                        x = layer if low else NX + layer
                        v_ext[c, pl.ds((x + 2) * PITCH + NY, NY), :] = value

    def stress_layer(step, x):
        row, base = place(x)
        main = pl.ds(pl.multiple_of(base, NY), NY)
        here = pl.ds(row, NY)
        mu = (TIME_STEP / 24.0) * modulus[here, :]
        lam = (TIME_STEP / 24.0) * lame[here, :]
        e_x = along_x(v_ext, 0, "B", base)
        e_y = along_y(v_ext, 1, "B", base)
        e_z = in_depth[2, here, :]
        dilation = lam * (e_x + e_y + e_z)
        twice = mu + mu
        rates = (
            dilation + twice * e_x,
            dilation + twice * e_y,
            dilation + twice * e_z,
            mu * (along_y(v_ext, 0, "F", base) + along_x(v_ext, 1, "F", base)),
            mu * (in_depth[0, here, :] + along_x(v_ext, 2, "F", base)),
            mu * (in_depth[1, here, :] + along_y(v_ext, 2, "F", base)),
        )
        s = [s_ext[f, main, :] + (rates[f] + inject[f, here, :]) for f in range(6)]
        pressure = (s[0] + s[1] + s[2]) * (1.0 / 3.0)
        d = [s[f] - pressure for f in range(3)]
        second = 0.5 * (d[0] * d[0] + d[1] * d[1] + d[2] * d[2])
        second = second + s[3] * s[3] + s[4] * s[4] + s[5] * s[5]
        limit = jnp.maximum(strength[here, :] - pressure * slope[here, :], 0.0)
        ratio = limit * lax.rsqrt(jnp.maximum(second, 0.0625))
        factor = jnp.where(eligible[here, :] == 1, jnp.minimum(ratio, 1.0), 1.0)
        new = [pressure + factor * d[f] for f in range(3)] + [factor * s[f] for f in (3, 4, 5)]
        for f in range(6):
            if step == STEPS - 1:
                stress_out[f, here, :] = new[f]
                if f < 3:
                    velocity_out[f, here, :] = v_ext[f, main, :]
            else:
                s_ext[f, main, :] = new[f]

    def deform(step):
        def body(k, _):
            for j in range(BENT):
                stress_layer(step, k * BENT + j)
            return _

        lax.fori_loop(0, NX // BENT, body, 0)

    def prepare():
        total_y = size_y * NY
        first = ((gx * NX) * total_y + gy * NY) * NZ
        within = row_of * NZ + lane

        def body(k, _):
            places = []
            for j in range(TILES):
                x = k * TILES + j
                here = pl.ds(pl.multiple_of(x * NY, NY), NY)
                which = zone[here, :]
                coh = jnp.full((NY, NZ), cohesion[0], jnp.float32)
                fri = jnp.full((NY, NZ), friction[0], jnp.float32)
                for z in range(1, 8):
                    hit = which == z
                    coh = jnp.where(hit, cohesion[z], coh)
                    fri = jnp.where(hit, friction[z], fri)
                strength[here, :] = coh * jnp.sqrt(1.0 - fri * fri)
                slope[here, :] = fri
                places.append((here, within + (first + x * (total_y * NZ))))
            for group in ((0, 1, 2), (3, 4, 5)):
                sums = [[zero] * len(group) for _ in places]
                for source in range(16):
                    moments = [moment[f, source] for f in group]
                    for j, (here, index) in enumerate(places):
                        hit = index == cell[source]
                        for f, value in enumerate(moments):
                            sums[j][f] = sums[j][f] + jnp.where(hit, value, 0.0)
                for j, (here, index) in enumerate(places):
                    for f, field in enumerate(group):
                        inject[field, here, :] = TIME_STEP * sums[j][f]
            return _

        lax.fori_loop(0, NX // TILES, body, 0)


    for step in range(STEPS):
        for d in ways["xy"]:
            sent[step, CORNER, d][...] = jnp.zeros((2 * NY, NZ), jnp.float32)
    for step in range(STEPS):
        if step == 0:
            for load in loads[:2]:
                load.wait()
            lax.fori_loop(0, NX // TILES, extend, 0)
            loads[2].wait()
        pack_stress(step)
        if step == 0:
            pack_corner(step)
            pack_flow_y(step)
            pack_flow_x(step)
            pl.semaphore_wait(barrier, expected)
            for axis in ways:
                up = ways[axis][-1]

                @pl.when(origin & there[axis][up])
                def _():
                    pl.semaphore_signal(
                        late_sem, inc=1, device_id=target[axis][up], device_id_type=MESH
                    )

        send(step, YS)
        if step:
            pack_corner(step)
        send(step, CORNER)
        send(step, XS)
        if step:
            pack_flow_y(step)
        send(step, YP)
        if step:
            pack_flow_x(step)
        send(step, XP)
        if step == 0:
            relay(step)
            turn(step)
        depth(s_ext, FORCE_Z)
        move(step)
        if step == 0:
            for load in loads[3:]:
                load.wait()
            prepare()
            send_origin()
        else:
            relay(step)
            turn(step)
        receive(step, XS)
        mend_x(step)
        depth(v_ext, FLOW_Z)
        receive(step, XP)
        receive(step, YS)
        mend_y(step)
        receive(step, CORNER)
        finish(step, "x")
        receive(step, YP)
        finish(step, "y")
        deform(step)
    for step, kind, d in MESSAGES:

        @pl.when(there[axis_of(kind)][d])
        def _():
            remote(step, kind, d).wait_send()

    for d, mine in turns:

        @pl.when(mine)
        def _():
            for step in range(STEPS):
                turned(step, d).wait_send()

    for d, p, mine in relays:

        @pl.when(mine)
        def _():
            for step, kind in PASSING:
                onward(step, kind, d, p).wait_send()


def write(velocity, stress, velocity_out, stress_out, sem):
    copies = [
        pltpu.make_async_copy(a.at[f], b.at[f], sem.at[at])
        for at, (a, b, f) in enumerate(
            [(velocity, velocity_out, f) for f in range(3)] + [(stress, stress_out, f) for f in range(6)]
        )
    ]
    for copy in copies:
        copy.start()
    for copy in copies:
        copy.wait()


def on_device(velocity, stress, lame, modulus, buoyancy, zone, eligible, *tables):
    rows = NX * NY
    flat = [a.reshape(a.shape[:-3] + (rows, NZ)) for a in (velocity, stress, lame, modulus, buoyancy, zone, eligible)]
    f32 = jnp.float32
    hbm = pl.BlockSpec(memory_space=pl.ANY)
    buffers = [
        pltpu.VMEM((message_rows(*m), NZ), f32) for m in MESSAGES
    ]
    block = pltpu.VMEM((rows, NZ), f32)
    whole = pltpu.VMEM((rows, NZ), jnp.int32)
    v, s = pl.pallas_call(
        kernel,
        out_shape=(
            pltpu.VMEM((3, rows, NZ), f32),
            pltpu.VMEM((6, rows, NZ), f32),
        ),
        in_specs=[hbm] * 11,
        out_specs=(pl.BlockSpec(memory_space=pltpu.VMEM),) * 2,
        scratch_shapes=[
            pltpu.VMEM((6, rows, NZ), f32),
            pltpu.VMEM((3, rows, NZ), f32),
            block,
            block,
            block,
            whole,
            whole,
            pltpu.SMEM((8,), f32),
            pltpu.SMEM((8,), f32),
            pltpu.SMEM((16,), jnp.int32),
            pltpu.SMEM((6, 16), f32),
            pltpu.VMEM((6, EXT, NZ), f32),
            pltpu.VMEM((3, EXT, NZ), f32),
            block,
            block,
            pltpu.VMEM((6, rows, NZ), f32),
            pltpu.VMEM((3, rows, NZ), f32),
            *buffers,
            *buffers,
            *[pltpu.VMEM((passing_rows(*m), NZ), f32) for m in PASSING],
            pltpu.VMEM((STEPS, 2, 2 * NY, NZ), f32),
            pltpu.SemaphoreType.DMA((11,)),
            pltpu.SemaphoreType.DMA((len(MESSAGES),)),
            pltpu.SemaphoreType.DMA((len(MESSAGES),)),
            pltpu.SemaphoreType.DMA((max(len(PASSING), 1),)),
            pltpu.SemaphoreType.DMA((max(len(PASSING), 1),)),
            pltpu.SemaphoreType.DMA((STEPS, 2)),
            pltpu.SemaphoreType.DMA((STEPS, 2)),
            pltpu.SemaphoreType.REGULAR,
        ],
        compiler_params=pltpu.CompilerParams(collective_id=0, has_side_effects=True),
    )(*flat, *tables)
    v, s = pl.pallas_call(
        write,
        out_shape=(
            jax.ShapeDtypeStruct((3, rows, NZ), f32),
            jax.ShapeDtypeStruct((6, rows, NZ), f32),
        ),
        in_specs=[hbm] * 2,
        out_specs=(hbm, hbm),
        scratch_shapes=[pltpu.SemaphoreType.DMA((9,))],
        compiler_params=pltpu.CompilerParams(vmem_limit_bytes=1 << 20),
    )(v, s)
    return v.reshape(velocity.shape), s.reshape(stress.shape)


def solution(mesh):
    wide, field, table = P(None, "gx", "gy", None), P("gx", "gy", None), P()
    return jax.shard_map(
        on_device,
        mesh=mesh,
        in_specs=(wide, wide) + (field,) * 5 + (table,) * 4,
        out_specs=(wide, wide),
        check_vma=False,
    )
```
